32 devices in a mesh: fsdp: 4 (over y, x), seq: 4 (over z), mlp: 2 (over core).
Axes of the slice: x: 2, y: 2, z: 4, core: 2. Of those that a mesh axis runs over, the one named last changes fastest.
Arguments:
- block_in: float32 [8, 1024, 2304], P(('fsdp', 'mlp'), 'seq'), may hold values from -6 to 6
- cotangent: float32 [8, 1024, 2304], P(('fsdp', 'mlp'), 'seq'), may hold values from -6 to 6
- attention_matrix: float32 [2304, 6144], P(('fsdp', 'seq', 'mlp')), may hold values from -0.25 to 0.25
- attention_first_moment: float32 [2304, 6144], P(('fsdp', 'seq', 'mlp')), may hold values from -48 to 48
- attention_second_moment: float32 [2304, 6144], P(('fsdp', 'seq', 'mlp')), may hold values from 5 to 500
- mlp_weight: float32 [3, 2304, 9216], P(None, 'fsdp', ('seq', 'mlp')), may hold values from -0.125 to 0.125
- first_mlp: float32 [3, 2304, 9216], P(None, 'fsdp', ('seq', 'mlp')), may hold values from -48 to 48
- second_mlp: float32 [3, 2304, 9216], P(None, 'fsdp', ('seq', 'mlp')), may hold values from 5 to 500
- norm_weight: float32 [4, 2304], P(None, ('fsdp', 'seq', 'mlp')), may hold values from -0.3 to 0.3
- first_norm: float32 [4, 2304], P(None, ('fsdp', 'seq', 'mlp')), may hold values from -48 to 48
- second_norm: float32 [4, 2304], P(None, ('fsdp', 'seq', 'mlp')), may hold values from 5 to 500
Outputs:
- block_out: float32 [8, 1024, 2304], P(('fsdp', 'mlp'), 'seq')
- input_grad: float32 [8, 1024, 2304], P(('fsdp', 'mlp'), 'seq')
- attn_grad: float32 [2304, 6144], P(('fsdp', 'seq', 'mlp'))
- attn_new: float32 [2304, 6144], P(('fsdp', 'seq', 'mlp'))
- first_attn_new: float32 [2304, 6144], P(('fsdp', 'seq', 'mlp'))
- second_attn_new: float32 [2304, 6144], P(('fsdp', 'seq', 'mlp'))
- mlp_grad: float32 [3, 2304, 9216], P(None, 'fsdp', ('seq', 'mlp'))
- mlp_new: float32 [3, 2304, 9216], P(None, 'fsdp', ('seq', 'mlp'))
- first_mlp_new: float32 [3, 2304, 9216], P(None, 'fsdp', ('seq', 'mlp'))
- second_mlp_new: float32 [3, 2304, 9216], P(None, 'fsdp', ('seq', 'mlp'))
- norm_grad: float32 [4, 2304], P(None, ('fsdp', 'seq', 'mlp'))
- norm_new: float32 [4, 2304], P(None, ('fsdp', 'seq', 'mlp'))
- first_norm_new: float32 [4, 2304], P(None, ('fsdp', 'seq', 'mlp'))
- second_norm_new: float32 [4, 2304], P(None, ('fsdp', 'seq', 'mlp'))
The draws below stay inside these ranges and needn't reach their ends.
All inputs are finite; a program needn't handle non-finite values.
Results may differ from the reference program's by a relative error of at most 0.03.
Values may be sent and summed in bfloat16 or wider, within the bound.
A program may use at most 384 MiB of HBM per device.

```python
import math
import jax
import jax.numpy as jnp
from jax import lax

MODEL_WIDTH = 2304
QUERY_HEADS = 8
KEY_VALUE_HEADS = 4
HEAD_SIZE = 256
FF = 9216
TOKENS_PER_SEQ = 1024
SEQ_DEV = 1
SEQS = 8
N_FSDP = 4
N_SEQ = 4
N_MLP = 2


def level_of(own_key, shape, shards, least, largest):
    def one(axis_at, parts):
        steps = jax.random.uniform(jax.random.fold_in(jax.random.fold_in(own_key, 6), axis_at), (parts,), jnp.float32, least / len(shards), largest / len(shards))
        return jnp.repeat(jnp.exp(steps), shape[axis_at] // parts).reshape((-1,) + (1,) * (len(shape) - axis_at - 1))

    gain = one(*shards[0])
    for cut in shards[1:]:
        gain = gain * one(*cut)
    return gain


def bell_draw(own_key, shape, width, reach, split=(), kind=jnp.bfloat16):
    drawn = width * jax.random.normal(own_key, shape, jnp.float32)
    if split:
        drawn = drawn * level_of(own_key, shape, split, -0.22, 0.18)
    return jnp.clip(drawn, -reach, reach).astype(kind)


def setup_inputs(seed: int = 0) -> dict:
    seeds = jax.random.split(jax.random.key(seed), 12)
    return {
        "block_in": bell_draw(seeds[0], (SEQS, TOKENS_PER_SEQ, MODEL_WIDTH), 1.0, 6.0, ((0, 8), (1, 4)), jnp.float32),
        "cotangent": bell_draw(seeds[1], (SEQS, TOKENS_PER_SEQ, MODEL_WIDTH), 1.0, 6.0, ((0, 8), (1, 4)), jnp.float32),
        "attention_matrix": bell_draw(seeds[2], (MODEL_WIDTH, 2 * QUERY_HEADS * HEAD_SIZE + 2 * KEY_VALUE_HEADS * HEAD_SIZE), (MODEL_WIDTH // 4) ** -0.5, 0.25, ((0, 32),), jnp.float32),
        "attention_first_moment": bell_draw(seeds[3], (MODEL_WIDTH, 2 * QUERY_HEADS * HEAD_SIZE + 2 * KEY_VALUE_HEADS * HEAD_SIZE), 8.0, 48.0, ((0, 32),), jnp.float32),
        "attention_second_moment": jnp.clip(jnp.exp(math.log(500.0) - 4.6051702 * jax.random.uniform(seeds[4], (MODEL_WIDTH, 2 * QUERY_HEADS * HEAD_SIZE + 2 * KEY_VALUE_HEADS * HEAD_SIZE), jnp.float32) ** level_of(seeds[4], (MODEL_WIDTH, 2 * QUERY_HEADS * HEAD_SIZE + 2 * KEY_VALUE_HEADS * HEAD_SIZE), ((0, 32),), -0.2, 0.2)), 5.0, 500.0),
        "mlp_weight": bell_draw(seeds[5], (3, MODEL_WIDTH, FF), MODEL_WIDTH ** -0.5, 0.125, ((1, 4), (2, 8)), jnp.float32),
        "first_mlp": bell_draw(seeds[6], (3, MODEL_WIDTH, FF), 8.0, 48.0, ((1, 4), (2, 8)), jnp.float32),
        "second_mlp": jnp.clip(jnp.exp(math.log(500.0) - 4.6051702 * jax.random.uniform(seeds[7], (3, MODEL_WIDTH, FF), jnp.float32) ** level_of(seeds[7], (3, MODEL_WIDTH, FF), ((1, 4), (2, 8)), -0.2, 0.2)), 5.0, 500.0),
        "norm_weight": jnp.clip(jax.random.uniform(seeds[8], (4, MODEL_WIDTH), jnp.float32, -0.3, 0.3) * level_of(seeds[8], (4, MODEL_WIDTH), ((1, 32),), -0.4, 0.0), -0.3, 0.3),
        "first_norm": bell_draw(seeds[9], (4, MODEL_WIDTH), 8.0, 48.0, ((1, 32),), jnp.float32),
        "second_norm": jnp.clip(jnp.exp(math.log(500.0) - 4.6051702 * jax.random.uniform(seeds[10], (4, MODEL_WIDTH), jnp.float32) ** level_of(seeds[10], (4, MODEL_WIDTH), ((1, 32),), -0.2, 0.2)), 5.0, 500.0),
    }


softcap = 50.0
norm_eps = 1e-06
beta_one = 0.9
beta_two = 0.95
adam_eps = 1e-08
learn_rate = 0.01
decay_rate = 0.1
step_count = 2

def matmul(left, right):
    return jnp.dot(left.astype(jnp.float32), right.astype(jnp.float32), preferred_element_type=jnp.float32)

def rounded(values):
    return lax.optimization_barrier(values.astype(jnp.bfloat16)).astype(jnp.float32)

def scale_rows(values):
    return lax.rsqrt(lax.optimization_barrier(jnp.mean(values * values, axis=-1, keepdims=True)) + norm_eps)

def norm_back(values, inverse, factor, upstream):
    normed = values * inverse
    scaled = upstream * factor
    inner_mean = lax.optimization_barrier(jnp.mean(scaled * normed, axis=-1, keepdims=True))
    return (inverse * (scaled - normed * inner_mean), lax.optimization_barrier(jnp.sum(upstream * normed, axis=0)))

def gelu_tanh(values):
    return jax.nn.gelu(values, approximate=True)

def adam_update(weight, gradient, first_moment, second_moment, decay_factor):
    first_new = beta_one * first_moment + (1.0 - beta_one) * gradient
    second_new = beta_two * second_moment + (1.0 - beta_two) * gradient * gradient
    first_hat = first_new / (1.0 - beta_one ** step_count)
    second_hat = second_new / (1.0 - beta_two ** step_count)
    weight_new = weight - learn_rate * (first_hat / (jnp.sqrt(second_hat) + adam_eps) + decay_factor * weight)
    return (weight_new, first_new, second_new)

def reference(block_in, cotangent, attention_matrix, attention_first_moment, attention_second_moment, mlp_weight, first_mlp, second_mlp, norm_weight, first_norm, second_norm):
    query_total_width = QUERY_HEADS * HEAD_SIZE
    key_value_width = KEY_VALUE_HEADS * HEAD_SIZE
    query_group_count = QUERY_HEADS // KEY_VALUE_HEADS
    piece_count = N_SEQ * N_MLP
    piece_width = FF // piece_count
    attn_bf = attention_matrix.astype(jnp.bfloat16)
    w_qkv = attn_bf[:, :query_total_width + 2 * key_value_width]
    w_out = attn_bf[:, query_total_width + 2 * key_value_width:]
    mlp_bf = mlp_weight.astype(jnp.bfloat16)
    perceptron_pieces = mlp_bf.astype(jnp.float32).reshape(3, MODEL_WIDTH, piece_count, piece_width)
    gain_rows = lax.optimization_barrier(norm_weight.astype(jnp.bfloat16))
    factor = 1.0 + gain_rows.astype(jnp.float32)
    row_index = lax.broadcasted_iota(jnp.int32, (TOKENS_PER_SEQ, TOKENS_PER_SEQ), 0)
    col_index = lax.broadcasted_iota(jnp.int32, (TOKENS_PER_SEQ, TOKENS_PER_SEQ), 1)
    causal = col_index <= row_index
    score_scale = HEAD_SIZE ** (-0.5)

    def one_sequence(carry, inputs):
        tok_rows, upstream = inputs
        inverse_in = scale_rows(tok_rows)
        normed_in = (tok_rows * inverse_in * factor[0]).astype(jnp.bfloat16)
        query_key_value_rows = matmul(normed_in, w_qkv).astype(jnp.bfloat16)
        queries = query_key_value_rows[:, :query_total_width].reshape(TOKENS_PER_SEQ, QUERY_HEADS, HEAD_SIZE)
        key_head_rows = jnp.repeat(query_key_value_rows[:, query_total_width:query_total_width + key_value_width].reshape(TOKENS_PER_SEQ, KEY_VALUE_HEADS, HEAD_SIZE), query_group_count, axis=1)
        value_head_rows = jnp.repeat(query_key_value_rows[:, query_total_width + key_value_width:].reshape(TOKENS_PER_SEQ, KEY_VALUE_HEADS, HEAD_SIZE), query_group_count, axis=1)
        raw_scores = jnp.einsum('qhc,khc->hqk', queries.astype(jnp.float32), key_head_rows.astype(jnp.float32)) * score_scale
        capped = softcap * jnp.tanh(raw_scores / softcap)
        logsum = jnp.log(lax.optimization_barrier(jnp.sum(jnp.where(causal, jnp.exp(capped), 0.0), axis=-1, keepdims=True)))
        prob_full = jnp.where(causal, jnp.exp(capped - logsum), 0.0)
        prob_bf = prob_full.astype(jnp.bfloat16)
        mixed_heads = jnp.einsum('hqk,khc->qhc', prob_bf.astype(jnp.float32), value_head_rows.astype(jnp.float32)).astype(jnp.bfloat16)
        mixed_rows = mixed_heads.reshape(TOKENS_PER_SEQ, query_total_width)
        projected = matmul(mixed_rows, w_out.T)
        inverse_one = scale_rows(projected)
        middle = tok_rows + projected * inverse_one * factor[1]
        inverse_two = scale_rows(middle)
        normed_mid = (middle * inverse_two * factor[2]).astype(jnp.bfloat16)
        gate_pre = matmul(normed_mid, mlp_bf[0])
        up_pre = matmul(normed_mid, mlp_bf[1])
        activated, gelu_back = jax.vjp(gelu_tanh, gate_pre)
        hidden_activation = (activated * up_pre).astype(jnp.bfloat16)
        feedforward_pieces = jnp.einsum('kvb,qvb->kvq', hidden_activation.astype(jnp.float32).reshape(TOKENS_PER_SEQ, piece_count, piece_width), perceptron_pieces[2])
        ffn_out = lax.optimization_barrier(jnp.sum(rounded(feedforward_pieces), axis=1))
        inverse_three = scale_rows(ffn_out)
        block_out = middle + ffn_out * inverse_three * factor[3]
        dffn, gain_three = norm_back(ffn_out, inverse_three, factor[3], upstream)
        dffn_bf = dffn.astype(jnp.bfloat16)
        dhidden = matmul(dffn_bf, mlp_bf[2])
        grad_down = matmul(dffn_bf.T, hidden_activation)
        gate_gradient = gelu_back(dhidden * up_pre)[0].astype(jnp.bfloat16)
        up_gradient_half = (dhidden * activated).astype(jnp.bfloat16)
        grad_gate = matmul(normed_mid.T, gate_gradient)
        grad_up = matmul(normed_mid.T, up_gradient_half)
        backward_pieces = jnp.einsum('kvb,qvb->kvq', gate_gradient.astype(jnp.float32).reshape(TOKENS_PER_SEQ, piece_count, piece_width), perceptron_pieces[0]) + jnp.einsum('kvb,qvb->kvq', up_gradient_half.astype(jnp.float32).reshape(TOKENS_PER_SEQ, piece_count, piece_width), perceptron_pieces[1])
        dnormed_mid = lax.optimization_barrier(jnp.sum(rounded(backward_pieces), axis=1))
        dmid_part, gain_two = norm_back(middle, inverse_two, factor[2], dnormed_mid)
        dmiddle = upstream + dmid_part
        dproj, gain_one = norm_back(projected, inverse_one, factor[1], dmiddle)
        dproj_bf = dproj.astype(jnp.bfloat16)
        dmixed = matmul(dproj_bf, w_out).astype(jnp.bfloat16)
        grad_out = matmul(dproj_bf.T, mixed_rows)
        dmixed_heads = dmixed.reshape(TOKENS_PER_SEQ, QUERY_HEADS, HEAD_SIZE)
        row_inner = lax.optimization_barrier(jnp.sum(dmixed_heads.astype(jnp.float32) * mixed_heads.astype(jnp.float32), axis=-1))
        dprob = jnp.einsum('qhc,khc->hqk', dmixed_heads.astype(jnp.float32), value_head_rows.astype(jnp.float32))
        dcapped = prob_full * (dprob - row_inner.T[:, :, None])
        dscore = (dcapped * (1.0 - capped / softcap * (capped / softcap)) * score_scale).astype(jnp.bfloat16)
        dquery = jnp.einsum('hqk,khc->qhc', dscore.astype(jnp.float32), key_head_rows.astype(jnp.float32)).astype(jnp.bfloat16)
        key_gradient_single = jnp.einsum('hqk,qhc->khc', dscore.astype(jnp.float32), queries.astype(jnp.float32)).astype(jnp.bfloat16)
        value_gradient_single = jnp.einsum('hqk,qhc->khc', prob_bf.astype(jnp.float32), dmixed_heads.astype(jnp.float32)).astype(jnp.bfloat16)
        key_gradient = lax.optimization_barrier(jnp.sum(key_gradient_single.astype(jnp.float32).reshape(TOKENS_PER_SEQ, KEY_VALUE_HEADS, query_group_count, HEAD_SIZE), axis=2)).astype(jnp.bfloat16)
        value_gradient = lax.optimization_barrier(jnp.sum(value_gradient_single.astype(jnp.float32).reshape(TOKENS_PER_SEQ, KEY_VALUE_HEADS, query_group_count, HEAD_SIZE), axis=2)).astype(jnp.bfloat16)
        dqkv = jnp.concatenate([dquery.reshape(TOKENS_PER_SEQ, query_total_width), key_gradient.reshape(TOKENS_PER_SEQ, key_value_width), value_gradient.reshape(TOKENS_PER_SEQ, key_value_width)], axis=1)
        dnormed_in = matmul(dqkv, w_qkv.T)
        grad_qkv = matmul(normed_in.T, dqkv)
        dinput_part, gain_zero = norm_back(tok_rows, inverse_in, factor[0], dnormed_in)
        input_grad = dmiddle + dinput_part
        attn_acc, mlp_acc, norm_acc = carry
        attn_acc = attn_acc + jnp.concatenate([grad_qkv, grad_out], axis=1)
        mlp_acc = mlp_acc + jnp.stack([grad_gate, grad_up, grad_down])
        norm_acc = norm_acc + jnp.stack([gain_zero, gain_one, gain_two, gain_three])
        return ((attn_acc, mlp_acc, norm_acc), (block_out, input_grad))

    def one_group(carry, inputs):
        attn_acc, mlp_total, norm_acc = carry
        inner_start = (attn_acc, jnp.zeros((3, MODEL_WIDTH, FF), jnp.float32), norm_acc)
        inner_end, group_outputs = lax.scan(one_sequence, inner_start, inputs)
        attn_acc, mlp_group, norm_acc = inner_end
        return ((attn_acc, mlp_total + rounded(mlp_group), norm_acc), group_outputs)
    group_size = N_MLP * SEQ_DEV
    start_carry = (jnp.zeros((MODEL_WIDTH, 2 * query_total_width + 2 * key_value_width), jnp.float32), jnp.zeros((3, MODEL_WIDTH, FF), jnp.float32), jnp.zeros((4, MODEL_WIDTH), jnp.float32))
    grouped_in = block_in.reshape(N_FSDP, group_size, TOKENS_PER_SEQ, MODEL_WIDTH)
    grouped_cot = cotangent.reshape(N_FSDP, group_size, TOKENS_PER_SEQ, MODEL_WIDTH)
    totals, outputs = lax.scan(one_group, start_carry, (grouped_in, grouped_cot))
    attn_grad, mlp_grad, norm_grad = totals
    block_out = outputs[0].reshape(SEQS, TOKENS_PER_SEQ, MODEL_WIDTH)
    input_grad = outputs[1].reshape(SEQS, TOKENS_PER_SEQ, MODEL_WIDTH)
    attn_new, first_attn_new, second_attn_new = adam_update(attention_matrix, attn_grad, attention_first_moment, attention_second_moment, decay_rate)
    mlp_new, first_mlp_new, second_mlp_new = adam_update(mlp_weight, mlp_grad, first_mlp, second_mlp, decay_rate)
    norm_new, first_norm_new, second_norm_new = adam_update(norm_weight, norm_grad, first_norm, second_norm, 0.0)
    return (block_out, input_grad, attn_grad, attn_new, first_attn_new, second_attn_new, mlp_grad, mlp_new, first_mlp_new, second_mlp_new, norm_grad, norm_new, first_norm_new, second_norm_new)
```

```python
import functools
import math

import jax
import jax.numpy as jnp
from jax import lax
from jax.experimental import pallas as pl
from jax.experimental.pallas import tpu as pltpu
from jax.sharding import PartitionSpec as P

QUERY_HEADS = 8
KEY_VALUE_HEADS = 4
HEAD_SIZE = 256


softcap = 50.0
norm_eps = 1e-06
beta_one = 0.9
beta_two = 0.95
adam_eps = 1e-08
learn_rate = 0.01
decay_rate = 0.1
step_count = 2
gelu_scale = math.sqrt(2.0 / math.pi)
gelu_cubic = 0.044715
mlp_chunks = 4


def scale_rows(values):
    return lax.rsqrt(jnp.mean(values * values, axis=-1, keepdims=True) + norm_eps)


def norm_back(values, inverse, factor, upstream):
    normed = values * inverse
    scaled = upstream * factor
    inner_mean = jnp.mean(scaled * normed, axis=-1, keepdims=True)
    return (inverse * (scaled - normed * inner_mean), jnp.sum(upstream * normed, axis=0))


def gelu_tanh(values):
    return jax.nn.gelu(values, approximate=True)


def adam_update(weight, gradient, first_moment, second_moment, decay_factor):
    first_new = beta_one * first_moment + (1.0 - beta_one) * gradient
    second_new = beta_two * second_moment + (1.0 - beta_two) * gradient * gradient
    first_hat = first_new / (1.0 - beta_one**step_count)
    second_hat = second_new / (1.0 - beta_two**step_count)
    weight_new = weight - learn_rate * (
        first_hat / (jnp.sqrt(second_hat) + adam_eps) + decay_factor * weight
    )
    return (weight_new, first_new, second_new)


def forward_scores(queries, key_head_rows, row_start):
    head_width = queries.shape[3]
    raw_scores = jnp.einsum(
        "sqlc,sklc->slqk", queries, key_head_rows, preferred_element_type=jnp.float32
    ) * head_width ** (-0.5)
    capped = softcap * jnp.tanh(raw_scores / softcap)
    shape_pair = (queries.shape[1], key_head_rows.shape[1])
    row_index = row_start + lax.broadcasted_iota(jnp.int32, shape_pair, 0)
    col_index = lax.broadcasted_iota(jnp.int32, shape_pair, 1)
    return (capped, col_index <= row_index)


def attend(queries, key_head_rows, value_head_rows, block_rows):
    sequence_count, length, head_count, head_width = queries.shape

    def one_block(block_index, carry_state):
        row_start = block_index * block_rows
        query_part = lax.dynamic_slice_in_dim(queries, row_start, block_rows, 1)
        capped, causal = forward_scores(query_part, key_head_rows, row_start)
        logsum = jnp.log(jnp.sum(jnp.where(causal, jnp.exp(capped), 0.0), axis=-1))
        prob_full = jnp.where(causal, jnp.exp(capped - logsum[..., None]), 0.0)
        prob_bf = prob_full.astype(jnp.bfloat16)
        mixed_part = jnp.einsum(
            "slqk,sklc->sqlc", prob_bf, value_head_rows, preferred_element_type=jnp.float32
        ).astype(jnp.bfloat16)
        outputs = lax.dynamic_update_slice_in_dim(carry_state[0], mixed_part, row_start, 1)
        totals = lax.dynamic_update_slice_in_dim(carry_state[1], logsum, row_start, 2)
        return (outputs, totals)

    start_state = (
        jnp.zeros(queries.shape, jnp.bfloat16),
        jnp.zeros((sequence_count, head_count, length), jnp.float32),
    )
    end_state = lax.fori_loop(0, length // block_rows, one_block, start_state)
    return (end_state[0], end_state[1], tuple(end_state[2:]))


def attend_back(queries, key_head_rows, value_head_rows, outputs, totals, upstream, block_rows):
    sequence_count, length, head_count, head_width = queries.shape
    row_inner = jnp.sum(upstream.astype(jnp.float32) * outputs.astype(jnp.float32), axis=-1)

    def one_block(block_index, carry_state):
        dquery, dkey_acc, dvalue_acc = carry_state
        row_start = block_index * block_rows
        query_part = lax.dynamic_slice_in_dim(queries, row_start, block_rows, 1)
        grad_part = lax.dynamic_slice_in_dim(upstream, row_start, block_rows, 1)
        inner_part = lax.dynamic_slice_in_dim(row_inner, row_start, block_rows, 1)
        logsum = lax.dynamic_slice_in_dim(totals, row_start, block_rows, 2)
        capped, causal = forward_scores(query_part, key_head_rows, row_start)
        prob_full = jnp.where(causal, jnp.exp(capped - logsum[..., None]), 0.0)
        dprob = jnp.einsum(
            "sqlc,sklc->slqk", grad_part, value_head_rows, preferred_element_type=jnp.float32
        )
        dcapped = prob_full * (dprob - jnp.transpose(inner_part, (0, 2, 1))[..., None])
        dscore = (
            dcapped * (1.0 - capped / softcap * (capped / softcap)) * head_width ** (-0.5)
        ).astype(jnp.bfloat16)
        dquery_part = jnp.einsum(
            "slqk,sklc->sqlc", dscore, key_head_rows, preferred_element_type=jnp.float32
        ).astype(jnp.bfloat16)
        dquery = lax.dynamic_update_slice_in_dim(dquery, dquery_part, row_start, 1)
        dkey_acc = dkey_acc + jnp.einsum(
            "slqk,sqlc->sklc", dscore, query_part, preferred_element_type=jnp.float32
        )
        dvalue_acc = dvalue_acc + jnp.einsum(
            "slqk,sqlc->sklc",
            prob_full.astype(jnp.bfloat16),
            grad_part,
            preferred_element_type=jnp.float32,
        )
        return (dquery, dkey_acc, dvalue_acc)

    start_state = (
        jnp.zeros(queries.shape, jnp.bfloat16),
        jnp.zeros(key_head_rows.shape, jnp.float32),
        jnp.zeros(value_head_rows.shape, jnp.float32),
    )
    dquery, dkey_acc, dvalue_acc = lax.fori_loop(0, length // block_rows, one_block, start_state)
    return (dquery, dkey_acc.astype(jnp.bfloat16), dvalue_acc.astype(jnp.bfloat16))


def on_device_generic(
    block_in,
    cotangent,
    attention_matrix,
    attention_first_moment,
    attention_second_moment,
    mlp_weight,
    first_mlp,
    second_mlp,
    norm_weight,
    first_norm,
    second_norm,
):
    sequence_count, token_length, feat_width = block_in.shape
    row_count = sequence_count * token_length
    query_total_width = QUERY_HEADS * HEAD_SIZE
    key_value_width = KEY_VALUE_HEADS * HEAD_SIZE
    query_group_count = QUERY_HEADS // KEY_VALUE_HEADS
    whole_attn, gain_rows = (
        lax.all_gather(
            attention_matrix.astype(jnp.bfloat16), ("fsdp", "seq", "mlp"), axis=0, tiled=True
        ),
        lax.all_gather(
            norm_weight.astype(jnp.bfloat16), ("fsdp", "seq", "mlp"), axis=1, tiled=True
        ),
    )
    factor = 1.0 + gain_rows.astype(jnp.float32)
    w_qkv = whole_attn[:, : query_total_width + 2 * key_value_width]
    w_out = whole_attn[:, query_total_width + 2 * key_value_width :]
    tok_rows = block_in.reshape(row_count, feat_width)
    upstream = cotangent.reshape(row_count, feat_width)
    inverse_in = scale_rows(tok_rows)
    normed_in = (tok_rows * inverse_in * factor[0]).astype(jnp.bfloat16)
    query_key_value_rows = jnp.dot(normed_in, w_qkv, preferred_element_type=jnp.float32).astype(
        jnp.bfloat16
    )
    queries = query_key_value_rows[:, :query_total_width].reshape(
        sequence_count, token_length, QUERY_HEADS, HEAD_SIZE
    )
    key_head_rows = jnp.repeat(
        query_key_value_rows[:, query_total_width : query_total_width + key_value_width].reshape(
            sequence_count, token_length, KEY_VALUE_HEADS, HEAD_SIZE
        ),
        query_group_count,
        axis=2,
    )
    value_head_rows = jnp.repeat(
        query_key_value_rows[:, query_total_width + key_value_width :].reshape(
            sequence_count, token_length, KEY_VALUE_HEADS, HEAD_SIZE
        ),
        query_group_count,
        axis=2,
    )
    query_h, key_h, value_h = (
        lax.all_to_all(queries, "seq", split_axis=2, concat_axis=1, tiled=True),
        lax.all_to_all(key_head_rows, "seq", split_axis=2, concat_axis=1, tiled=True),
        lax.all_to_all(value_head_rows, "seq", split_axis=2, concat_axis=1, tiled=True),
    )
    block_rows = min(512, query_h.shape[1])
    mixed_h, totals, saved_state = attend(query_h, key_h, value_h, block_rows)
    mixed = lax.all_to_all(mixed_h, "seq", split_axis=1, concat_axis=2, tiled=True)
    mixed_rows = mixed.reshape(row_count, query_total_width)
    projected = jnp.einsum("rc,dc->rd", mixed_rows, w_out, preferred_element_type=jnp.float32)
    inverse_one = scale_rows(projected)
    middle = tok_rows + projected * inverse_one * factor[1]
    inverse_two = scale_rows(middle)
    normed_mid = (middle * inverse_two * factor[2]).astype(jnp.bfloat16)
    mlp_rows = lax.all_gather(normed_mid, ("seq", "mlp"), axis=0, tiled=True)
    whole_mlp = lax.all_gather(mlp_weight.astype(jnp.bfloat16), "fsdp", axis=1, tiled=True)
    gate_pre = jnp.dot(mlp_rows, whole_mlp[0], preferred_element_type=jnp.float32)
    up_pre = jnp.dot(mlp_rows, whole_mlp[1], preferred_element_type=jnp.float32)
    activated, gelu_back = jax.vjp(gelu_tanh, gate_pre)
    hidden_activation = (activated * up_pre).astype(jnp.bfloat16)
    ffn_part = jnp.einsum(
        "rf,df->rd", hidden_activation, whole_mlp[2], preferred_element_type=jnp.float32
    )
    ffn_out = lax.psum_scatter(
        ffn_part.astype(jnp.bfloat16), ("seq", "mlp"), scatter_dimension=0, tiled=True
    ).astype(jnp.float32)
    inverse_three = scale_rows(ffn_out)
    block_out = middle + ffn_out * inverse_three * factor[3]
    dffn, gain_three = norm_back(ffn_out, inverse_three, factor[3], upstream)
    dffn_rows = lax.all_gather(dffn.astype(jnp.bfloat16), ("seq", "mlp"), axis=0, tiled=True)
    dhidden = jnp.dot(dffn_rows, whole_mlp[2], preferred_element_type=jnp.float32)
    grad_down = jnp.einsum(
        "rd,rf->df", dffn_rows, hidden_activation, preferred_element_type=jnp.float32
    )
    gate_gradient = gelu_back(dhidden * up_pre)[0].astype(jnp.bfloat16)
    up_gradient_half = (dhidden * activated).astype(jnp.bfloat16)
    grad_gate = jnp.einsum("rd,rf->df", mlp_rows, gate_gradient, preferred_element_type=jnp.float32)
    grad_up = jnp.einsum(
        "rd,rf->df", mlp_rows, up_gradient_half, preferred_element_type=jnp.float32
    )
    dnormed_part = jnp.einsum(
        "rf,df->rd", gate_gradient, whole_mlp[0], preferred_element_type=jnp.float32
    ) + jnp.einsum("rf,df->rd", up_gradient_half, whole_mlp[1], preferred_element_type=jnp.float32)
    mlp_grad = lax.psum_scatter(
        jnp.stack([grad_gate, grad_up, grad_down]).astype(jnp.bfloat16),
        "fsdp",
        scatter_dimension=1,
        tiled=True,
    ).astype(jnp.float32)
    dnormed_mid = lax.psum_scatter(
        dnormed_part.astype(jnp.bfloat16), ("seq", "mlp"), scatter_dimension=0, tiled=True
    ).astype(jnp.float32)
    dmid_part, gain_two = norm_back(middle, inverse_two, factor[2], dnormed_mid)
    dmiddle = upstream + dmid_part
    dproj, gain_one = norm_back(projected, inverse_one, factor[1], dmiddle)
    dproj_bf = dproj.astype(jnp.bfloat16)
    dmixed = jnp.dot(dproj_bf, w_out, preferred_element_type=jnp.float32).astype(jnp.bfloat16)
    dmixed_h = lax.all_to_all(
        dmixed.reshape(sequence_count, token_length, QUERY_HEADS, HEAD_SIZE),
        "seq",
        split_axis=2,
        concat_axis=1,
        tiled=True,
    )
    dquery_h, dkey_h, dvalue_h = attend_back(
        query_h, key_h, value_h, mixed_h, totals, dmixed_h, block_rows
    )
    dquery, key_gradient_single, value_gradient_single = (
        lax.all_to_all(dquery_h, "seq", split_axis=1, concat_axis=2, tiled=True),
        lax.all_to_all(dkey_h, "seq", split_axis=1, concat_axis=2, tiled=True),
        lax.all_to_all(dvalue_h, "seq", split_axis=1, concat_axis=2, tiled=True),
    )
    key_gradient = jnp.sum(
        key_gradient_single.astype(jnp.float32).reshape(
            sequence_count, token_length, KEY_VALUE_HEADS, query_group_count, HEAD_SIZE
        ),
        axis=3,
    ).astype(jnp.bfloat16)
    value_gradient = jnp.sum(
        value_gradient_single.astype(jnp.float32).reshape(
            sequence_count, token_length, KEY_VALUE_HEADS, query_group_count, HEAD_SIZE
        ),
        axis=3,
    ).astype(jnp.bfloat16)
    dqkv = jnp.concatenate(
        [
            dquery.reshape(row_count, query_total_width),
            key_gradient.reshape(row_count, key_value_width),
            value_gradient.reshape(row_count, key_value_width),
        ],
        axis=1,
    )
    dnormed_in = jnp.einsum("rc,dc->rd", dqkv, w_qkv, preferred_element_type=jnp.float32)
    dinput_part, gain_zero = norm_back(tok_rows, inverse_in, factor[0], dnormed_in)
    input_grad = dmiddle + dinput_part
    fsdp_count = lax.axis_size("fsdp")
    seq_count = lax.axis_size("seq")
    mlp_count = lax.axis_size("mlp")
    seq_index = lax.axis_index("seq")
    row_share = feat_width // (fsdp_count * seq_count * mlp_count)
    whole_xn, whole_dqkv, whole_dproj, whole_mixed = (
        lax.all_gather(normed_in, "seq", axis=0, tiled=True),
        lax.all_gather(dqkv, "seq", axis=0, tiled=True),
        lax.all_gather(dproj_bf, "seq", axis=0, tiled=True),
        lax.all_gather(mixed_rows, "seq", axis=0, tiled=True),
    )

    def own_columns(values):
        parted = values.reshape(values.shape[0], fsdp_count, seq_count, mlp_count, row_share)
        picked = lax.dynamic_index_in_dim(parted, seq_index, 2, keepdims=False)
        return picked.reshape(values.shape[0], fsdp_count * mlp_count * row_share)

    xn_own = own_columns(whole_xn)
    dproj_own = own_columns(whole_dproj)
    grad_rows = jnp.concatenate(
        [
            jnp.einsum("tr,tc->rc", xn_own, whole_dqkv, preferred_element_type=jnp.float32),
            jnp.einsum("tr,tc->rc", dproj_own, whole_mixed, preferred_element_type=jnp.float32),
        ],
        axis=1,
    )
    attn_grad = lax.psum_scatter(
        grad_rows.astype(jnp.bfloat16), ("fsdp", "mlp"), scatter_dimension=0, tiled=True
    ).astype(jnp.float32)
    norm_grad = lax.psum_scatter(
        jnp.stack([gain_zero, gain_one, gain_two, gain_three]),
        ("fsdp", "seq", "mlp"),
        scatter_dimension=1,
        tiled=True,
    )
    attn_new, first_attn_new, second_attn_new = adam_update(
        attention_matrix, attn_grad, attention_first_moment, attention_second_moment, decay_rate
    )
    mlp_new, first_mlp_new, second_mlp_new = adam_update(
        mlp_weight, mlp_grad, first_mlp, second_mlp, decay_rate
    )
    norm_new, first_norm_new, second_norm_new = adam_update(
        norm_weight, norm_grad, first_norm, second_norm, 0.0
    )
    return (
        block_out.reshape(block_in.shape),
        input_grad.reshape(block_in.shape),
        attn_grad,
        attn_new,
        first_attn_new,
        second_attn_new,
        mlp_grad,
        mlp_new,
        first_mlp_new,
        second_mlp_new,
        norm_grad,
        norm_new,
        first_norm_new,
        second_norm_new,
    )


MESH = pl.DeviceIdType.MESH
AXES = ("fsdp", "seq", "mlp")


def exchange_kernel(sizes, mine_ref, out_ref, send_sem, recv_sem):
    n_fsdp, n_seq, n_mlp = sizes
    count = n_fsdp * n_seq * n_mlp
    me = (lax.axis_index("fsdp") * n_seq + lax.axis_index("seq")) * n_mlp + lax.axis_index("mlp")
    slots = mine_ref.shape[0]

    def place(index):
        return (index // (n_seq * n_mlp), (index // n_mlp) % n_seq, index % n_mlp)

    barrier = pltpu.get_barrier_semaphore()

    @pl.loop(1, count)
    def _(step):
        pl.semaphore_signal(barrier, inc=1, device_id=place((me + step) % count), device_id_type=MESH)

    pl.semaphore_wait(barrier, count - 1)

    def copy_to(step):
        to = (me + step) % count
        return pltpu.make_async_remote_copy(
            src_ref=mine_ref.at[to % slots],
            dst_ref=out_ref.at[me],
            send_sem=send_sem.at[step],
            recv_sem=recv_sem.at[step],
            device_id=place(to),
            device_id_type=MESH,
        )

    @pl.loop(1, count)
    def _(step):
        copy_to(step).start()

    out_ref[pl.ds(me, 1)] = mine_ref[pl.ds(me % slots, 1)]

    @pl.loop(1, count)
    def _(step):
        copy_to(step).wait()


def exchange(sizes, mine, collective_id):
    count = sizes[0] * sizes[1] * sizes[2]
    return pl.pallas_call(
        functools.partial(exchange_kernel, sizes),
        out_shape=jax.ShapeDtypeStruct((count,) + mine.shape[1:], mine.dtype),
        in_specs=[pl.BlockSpec(memory_space=pltpu.VMEM)],
        out_specs=pl.BlockSpec(memory_space=pltpu.VMEM),
        scratch_shapes=[pltpu.SemaphoreType.DMA((count,)), pltpu.SemaphoreType.DMA((count,))],
        compiler_params=pltpu.CompilerParams(collective_id=collective_id, has_side_effects=True),
    )(mine)


def neighbour_barrier(seq_count, at, up, down, sibling):
    barrier = pltpu.get_barrier_semaphore()

    @pl.when(at < seq_count - 1)
    def _():
        pl.semaphore_signal(barrier, inc=1, device_id=up, device_id_type=MESH)

    @pl.when(at > 0)
    def _():
        pl.semaphore_signal(barrier, inc=1, device_id=down, device_id_type=MESH)

    peers = jnp.where(at < seq_count - 1, 1, 0) + jnp.where(at > 0, 1, 0)
    if sibling is not None:
        pl.semaphore_signal(barrier, inc=1, device_id=sibling, device_id_type=MESH)
        peers = peers + 1
    pl.semaphore_wait(barrier, peers)


class RowGather:
    def __init__(self, n, own, whole, send_sem, recv_sem):
        self.n, self.own, self.whole = n, own, whole
        self.send_sem, self.recv_sem = send_sem, recv_sem
        self.fsdp, self.at, self.core = (
            lax.axis_index("fsdp"),
            lax.axis_index("seq"),
            lax.axis_index("mlp"),
        )
        self.up = (self.fsdp, lax.rem(self.at + 1, n), self.core)
        self.down = (self.fsdp, lax.rem(self.at + n - 1, n), self.core)
        self.sibling = (self.fsdp, self.at, 1 - self.core)

    def copy(self, chunk, block, way, own=False):
        slot = self.core * self.n + block
        return pltpu.make_async_remote_copy(
            src_ref=self.own.at[chunk] if own else self.whole.at[chunk, slot],
            dst_ref=self.whole.at[chunk, slot],
            send_sem=self.send_sem.at[chunk, way, block],
            recv_sem=self.recv_sem.at[chunk, slot],
            device_id=(self.up, self.down, self.sibling)[way],
            device_id_type=MESH,
        )

    def arrival(self, chunk, slot):
        return pltpu.make_async_remote_copy(
            src_ref=self.own.at[chunk],
            dst_ref=self.whole.at[chunk, slot],
            send_sem=self.send_sem.at[chunk, 0, 0],
            recv_sem=self.recv_sem.at[chunk, slot],
            device_id=self.sibling,
            device_id_type=MESH,
        )

    def begin(self, chunk):
        @pl.when(self.at < self.n - 1)
        def _():
            self.copy(chunk, self.at, 0, True).start()

        @pl.when(self.at > 0)
        def _():
            self.copy(chunk, self.at, 1, True).start()

        self.copy(chunk, self.at, 2, True).start()

    def step(self, chunk, hop):
        below, above = self.at - hop, self.at + hop

        @pl.when(below >= 0)
        def _():
            self.arrival(chunk, self.core * self.n + below).wait_recv()

            @pl.when(self.at < self.n - 1)
            def _():
                self.copy(chunk, below, 0).start()

            self.copy(chunk, below, 2).start()

        @pl.when(above < self.n)
        def _():
            self.arrival(chunk, self.core * self.n + above).wait_recv()

            @pl.when(self.at > 0)
            def _():
                self.copy(chunk, above, 1).start()

            self.copy(chunk, above, 2).start()

    def finish(self, chunk):
        for block in range(self.n):
            self.arrival(chunk, (1 - self.core) * self.n + block).wait_recv()

    def drain(self, chunk):
        for block in range(self.n):

            @pl.when((block <= self.at) & (self.at < self.n - 1))
            def _():
                self.copy(chunk, block, 0).wait_send()

            @pl.when((block >= self.at) & (self.at > 0))
            def _():
                self.copy(chunk, block, 1).wait_send()

            self.copy(chunk, block, 2).wait_send()


class RowScatter:
    def __init__(self, n, total, held, send_sem, recv_sem):
        self.n, self.total, self.held = n, total, held
        self.send_sem, self.recv_sem = send_sem, recv_sem
        self.fsdp, self.at, self.core = (
            lax.axis_index("fsdp"),
            lax.axis_index("seq"),
            lax.axis_index("mlp"),
        )
        self.up = (self.fsdp, lax.rem(self.at + 1, n), self.core)
        self.down = (self.fsdp, lax.rem(self.at + n - 1, n), self.core)

    def copy(self, chunk, block, way):
        slot = block
        if way == 1:
            slot = jnp.where(block == self.at - 1, self.n, block)
        return pltpu.make_async_remote_copy(
            src_ref=self.total.at[chunk, block],
            dst_ref=self.held.at[chunk, slot],
            send_sem=self.send_sem.at[chunk, way, block],
            recv_sem=self.recv_sem.at[chunk, slot],
            device_id=(self.up, self.down)[way],
            device_id_type=MESH,
        )

    def arrive(self, chunk, slot):
        pltpu.make_async_remote_copy(
            src_ref=self.total.at[chunk, 0],
            dst_ref=self.held.at[chunk, slot],
            send_sem=self.send_sem.at[chunk, 0, 0],
            recv_sem=self.recv_sem.at[chunk, slot],
            device_id=self.up,
            device_id_type=MESH,
        ).wait_recv()

    def add(self, chunk, block):
        self.arrive(chunk, block)
        self.total[chunk, block] = (
            self.total[chunk, block].astype(jnp.float32)
            + self.held[chunk, block].astype(jnp.float32)
        ).astype(jnp.bfloat16)

    def step(self, chunk, wave):
        far = self.n - 1 - self.at

        @pl.when(self.at < wave)
        def _():
            block = self.n - wave + self.at

            @pl.when(self.at > 0)
            def _():
                self.add(chunk, block)

            self.copy(chunk, block, 0).start()

        @pl.when(far < wave)
        def _():
            block = wave - 1 - far

            @pl.when(far > 0)
            def _():
                self.add(chunk, block)

            self.copy(chunk, block, 1).start()

    def finish(self, chunk, store):
        own = self.total[chunk, self.at].astype(jnp.float32)
        last = self.n - 1

        @pl.when(self.at == 0)
        def _():
            self.arrive(chunk, self.n)
            store(own + self.held[chunk, self.n].astype(jnp.float32))

        @pl.when(self.at == last)
        def _():
            self.arrive(chunk, self.at)
            store(own + self.held[chunk, self.at].astype(jnp.float32))

        @pl.when((self.at > 0) & (self.at < last))
        def _():
            self.arrive(chunk, self.at)
            self.arrive(chunk, self.n)
            store(
                own
                + self.held[chunk, self.at].astype(jnp.float32)
                + self.held[chunk, self.n].astype(jnp.float32)
            )

    def drain(self, chunk):
        for block in range(self.n):

            @pl.when(block > self.at)
            def _():
                self.copy(chunk, block, 0).wait_send()

            @pl.when(block < self.at)
            def _():
                self.copy(chunk, block, 1).wait_send()


def column_tiles(width, tile):
    return [(start, min(tile, width - start)) for start in range(0, width, tile)]


def mlp_kernel(
    forward,
    n,
    own,
    weights,
    saved_in,
    whole_out,
    saved_out,
    result,
    whole,
    w_vmem,
    loaded,
    stored,
    partner,
    arrived,
    total,
    held,
    gather_send,
    gather_recv,
    pair_send,
    pair_recv,
    scatter_send,
    scatter_recv,
    own_sem,
    w_sem,
    load_sem,
    store_sem,
    whole_sem,
):
    chunks, rows, width = own.shape
    hidden = w_vmem[0].shape[1]
    line_rows = n * rows
    all_rows = 2 * line_rows
    gather = RowGather(n, own, whole, gather_send, gather_recv)
    scatter = RowScatter(n, total, held, scatter_send, scatter_recv)
    core = gather.core

    w_copies = [
        pltpu.make_async_copy(w, v, w_sem.at[i]) for i, (w, v) in enumerate(zip(weights, w_vmem))
    ]
    for copy in w_copies:
        copy.start()
    neighbour_barrier(n, gather.at, gather.up, gather.down, gather.sibling)
    gather.begin(0)
    own_copies = [
        pltpu.make_async_copy(own.at[c], whole.at[c, core * n + gather.at], own_sem.at[c])
        for c in range(chunks)
    ]
    for copy in own_copies:
        copy.start()

    def load(chunk, slot):
        return [
            pltpu.make_async_copy(ref.at[chunk], buf.at[slot], load_sem.at[i, slot])
            for i, (ref, buf) in enumerate(zip(saved_in, loaded))
        ]

    def store(chunk, slot):
        return [
            pltpu.make_async_copy(buf.at[slot], ref.at[chunk], store_sem.at[i, slot])
            for i, (ref, buf) in enumerate(zip(saved_out, stored))
        ]

    def keep(chunk):
        return pltpu.make_async_copy(whole.at[chunk], whole_out.at[chunk], whole_sem.at[chunk])

    def swap(chunk, slot):
        return pltpu.make_async_remote_copy(
            src_ref=partner.at[slot],
            dst_ref=arrived.at[chunk],
            send_sem=pair_send.at[slot],
            recv_sem=pair_recv.at[chunk],
            device_id=gather.sibling,
            device_id_type=MESH,
        )

    for copy in load(0, 0):
        copy.start()
    for hop in range(1, n):
        gather.step(0, hop)
    for copy in own_copies + w_copies:
        copy.wait()
    gather.finish(0)

    def pair_sum(chunk):
        swap(chunk, 0).wait_recv()
        for block in range(n):
            total[chunk, block] = (
                total[chunk, block].astype(jnp.float32)
                + arrived[chunk, block].astype(jnp.float32)
            ).astype(jnp.bfloat16)

    def finish_chunk(chunk):
        def write(value):
            result[chunk] = value

        scatter.finish(chunk, write)

    tiles = column_tiles(hidden, 256)
    groups = [tiles[: len(tiles) // 2], tiles[len(tiles) // 2 :]]

    @pl.loop(0, chunks)
    def _(chunk):
        slot = lax.rem(chunk, 2)
        more = chunk + 1 < chunks
        behind = chunk > 0

        keep(chunk).start()
        for copy in load(chunk, slot):
            copy.wait()

        @pl.when(more)
        def _():
            gather.begin(chunk + 1)
            for copy in load(chunk + 1, 1 - slot):
                copy.start()

        @pl.when(chunk > 1)
        def _():
            for copy in store(chunk, slot):
                copy.wait()

        def first_half(part):
            for start, size in groups[part]:
                cols = slice(start, start + size)
                tokens = whole[chunk].reshape(all_rows, width)
                if forward:
                    gate = jnp.dot(tokens, w_vmem[0][:, cols], preferred_element_type=jnp.float32)
                    up = jnp.dot(tokens, w_vmem[1][:, cols], preferred_element_type=jnp.float32)
                    inner = gelu_scale * (gate + gelu_cubic * gate * gate * gate)
                    wave = jnp.tanh(inner)
                    half = 0.5 * (1.0 + wave)
                    gelu = gate * half
                    slope = half + 0.5 * gate * (1.0 - wave * wave) * gelu_scale * (
                        1.0 + 3.0 * gelu_cubic * gate * gate
                    )
                    stored[0][slot, :, cols] = (gelu * up).astype(jnp.bfloat16)
                    stored[1][slot, :, cols] = gelu.astype(jnp.bfloat16)
                    stored[2][slot, :, cols] = (slope * up).astype(jnp.bfloat16)
                else:
                    dact = jnp.dot(tokens, w_vmem[2][:, cols], preferred_element_type=jnp.float32)
                    stored[0][slot, :, cols] = (
                        dact * loaded[1][slot, :, cols].astype(jnp.float32)
                    ).astype(jnp.bfloat16)
                    stored[1][slot, :, cols] = (
                        dact * loaded[0][slot, :, cols].astype(jnp.float32)
                    ).astype(jnp.bfloat16)

        def second_half(line, put):
            part = pl.ds(pl.multiple_of(line * line_rows, line_rows), line_rows)
            for start, size in column_tiles(width, 768):
                cols = slice(start, start + size)

                def back(left, right):
                    return lax.dot_general(
                        left[slot, part, :],
                        right[cols, :],
                        (((1,), (1,)), ((), ())),
                        preferred_element_type=jnp.float32,
                    )

                if forward:
                    value = back(stored[0], w_vmem[2])
                else:
                    value = back(stored[0], w_vmem[0]) + back(stored[1], w_vmem[1])
                put(cols, value.astype(jnp.bfloat16).reshape(n, rows, size))

        def between(step):
            @pl.when(more)
            def _():
                if step < n:
                    gather.step(chunk + 1, step)
                else:
                    gather.finish(chunk + 1)

            @pl.when(behind)
            def _():
                if step < n:
                    scatter.step(chunk - 1, step)
                else:
                    finish_chunk(chunk - 1)

        @pl.when(behind)
        def _():
            pair_sum(chunk - 1)

        waits = list(range(1, n + 1))
        first_half(0)
        between(waits.pop(0))
        first_half(1)
        for copy in store(chunk, slot):
            copy.start()
        if len(waits) > 1:
            between(waits.pop(0))

        @pl.when(chunk > 1)
        def _():
            swap(chunk, slot).wait_send()

        def put_partner(cols, value):
            partner[slot, :, :, cols] = value

        second_half(1 - core, put_partner)
        while len(waits) > 1:
            between(waits.pop(0))
        swap(chunk, slot).start()

        def put_total(cols, value):
            total[chunk, :, :, cols] = value

        second_half(core, put_total)
        between(waits.pop(0))

    last = chunks - 1
    pair_sum(last)
    for wave in range(1, n):
        scatter.step(last, wave)
    finish_chunk(last)

    for chunk in range(chunks):
        gather.drain(chunk)
        scatter.drain(chunk)
        keep(chunk).wait()
    for chunk in range(max(chunks - 2, 0), chunks):
        swap(chunk, chunk % 2).wait_send()
        for copy in store(chunk, chunk % 2):
            copy.wait()


def mlp_half(forward, n, own, weights, saved, collective_id):
    chunks, rows, width = own.shape
    hidden = weights[0].shape[1]
    all_rows = 2 * n * rows
    outs = 3 if forward else 2
    hidden_shape = jax.ShapeDtypeStruct((chunks, all_rows, hidden), jnp.bfloat16)

    def kernel(*refs):
        refs = list(refs)

        def take(count):
            taken = refs[:count]
            del refs[:count]
            return taken

        (own_ref,) = take(1)
        weight_refs = take(3)
        saved_refs = take(len(saved))
        (whole_out,) = take(1)
        saved_out = take(outs)
        (result,) = take(1)
        (whole,) = take(1)
        w_vmem = take(3)
        loaded = take(len(saved))
        stored = take(outs)
        mlp_kernel(
            forward,
            n,
            own_ref,
            weight_refs,
            saved_refs,
            whole_out,
            saved_out,
            result,
            whole,
            w_vmem,
            loaded,
            stored,
            *refs,
        )

    hbm = pl.BlockSpec(memory_space=pl.ANY)
    vmem = pl.BlockSpec(memory_space=pltpu.VMEM)
    bf16 = jnp.bfloat16
    flops = 2 * chunks * all_rows * width * hidden * 3
    return pl.pallas_call(
        kernel,
        name="mlp_forward" if forward else "mlp_backward",
        out_shape=(
            [jax.ShapeDtypeStruct((chunks, 2 * n, rows, width), bf16)]
            + [hidden_shape] * outs
            + [jax.ShapeDtypeStruct((chunks, rows, width), jnp.float32)]
        ),
        in_specs=[vmem] + [hbm] * (3 + len(saved)),
        out_specs=[hbm] * (1 + outs) + [vmem],
        scratch_shapes=(
            [pltpu.VMEM((chunks, 2 * n, rows, width), bf16)]
            + [pltpu.VMEM((width, hidden), bf16)] * 3
            + [pltpu.VMEM((2, all_rows, hidden), bf16)] * (len(saved) + outs)
            + [
                pltpu.VMEM((2, n, rows, width), bf16),
                pltpu.VMEM((chunks, n, rows, width), bf16),
                pltpu.VMEM((chunks, n, rows, width), bf16),
                pltpu.VMEM((chunks, n + 1, rows, width), bf16),
                pltpu.SemaphoreType.DMA((chunks, 3, n)),
                pltpu.SemaphoreType.DMA((chunks, 2 * n)),
                pltpu.SemaphoreType.DMA((2,)),
                pltpu.SemaphoreType.DMA((chunks,)),
                pltpu.SemaphoreType.DMA((chunks, 2, n)),
                pltpu.SemaphoreType.DMA((chunks, n + 1)),
                pltpu.SemaphoreType.DMA((chunks,)),
                pltpu.SemaphoreType.DMA((3,)),
                pltpu.SemaphoreType.DMA((max(len(saved), 1), 2)),
                pltpu.SemaphoreType.DMA((outs, 2)),
                pltpu.SemaphoreType.DMA((chunks,)),
            ]
        ),
        compiler_params=pltpu.CompilerParams(
            collective_id=collective_id, has_side_effects=True, vmem_limit_bytes=60 << 20
        ),
        cost_estimate=pl.CostEstimate(
            flops=flops, bytes_accessed=2 * 3 * width * hidden, transcendentals=0
        ),
    )(own, *weights, *saved)


def on_device(
    sizes,
    block_in,
    cotangent,
    attention_matrix,
    attention_first_moment,
    attention_second_moment,
    mlp_weight,
    first_mlp,
    second_mlp,
    norm_weight,
    first_norm,
    second_norm,
):
    n_fsdp, n_seq, n_mlp = sizes
    count = n_fsdp * n_seq * n_mlp
    sequence_count, token_length, feat_width = block_in.shape
    row_count = sequence_count * token_length
    seq_rows = n_seq * row_count
    query_total_width = QUERY_HEADS * HEAD_SIZE
    key_value_width = KEY_VALUE_HEADS * HEAD_SIZE
    group = QUERY_HEADS // KEY_VALUE_HEADS
    heads = QUERY_HEADS // n_seq
    kv_heads = KEY_VALUE_HEADS // n_seq
    own_q = heads * HEAD_SIZE
    own_kv = kv_heads * HEAD_SIZE
    own_width = own_q + 2 * own_kv
    share = attention_matrix.shape[0]

    tok_rows = block_in.reshape(row_count, feat_width)
    upstream = cotangent.reshape(row_count, feat_width)

    gain_tile = jnp.zeros((1, 8, 128), jnp.float32)
    gain_tile = gain_tile.at[0, : norm_weight.shape[0], : norm_weight.shape[1]].set(
        norm_weight.astype(jnp.bfloat16).astype(jnp.float32)
    )
    gain_tiles = exchange(sizes, gain_tile, 0)
    gains = gain_tiles[:, : norm_weight.shape[0], : norm_weight.shape[1]]
    factor = 1.0 + jnp.transpose(gains, (1, 0, 2)).reshape(norm_weight.shape[0], feat_width)

    attn_bf = attention_matrix.astype(jnp.bfloat16)
    head_parts = jnp.concatenate(
        [
            attn_bf[:, :query_total_width].reshape(share, n_seq, own_q),
            attn_bf[:, query_total_width : query_total_width + key_value_width].reshape(
                share, n_seq, own_kv
            ),
            attn_bf[
                :, query_total_width + key_value_width : query_total_width + 2 * key_value_width
            ].reshape(share, n_seq, own_kv),
        ],
        axis=2,
    )
    head_cols = lax.all_to_all(
        jnp.transpose(head_parts, (1, 0, 2)), "seq", split_axis=0, concat_axis=0, tiled=True
    )
    w_qkv = lax.all_gather(head_cols, ("fsdp", "mlp"), axis=0, tiled=False)
    w_qkv = jnp.transpose(
        w_qkv.reshape(n_fsdp, n_mlp, n_seq, share, own_width), (0, 2, 1, 3, 4)
    ).reshape(feat_width, own_width)
    w_out = lax.all_gather(
        attn_bf[:, query_total_width + 2 * key_value_width :], AXES, axis=0, tiled=True
    )

    inverse_in = scale_rows(tok_rows)
    normed_in = (tok_rows * inverse_in * factor[0]).astype(jnp.bfloat16)
    whole_xn = lax.all_gather(normed_in, "seq", axis=0, tiled=True)
    qkv = jnp.dot(whole_xn, w_qkv, preferred_element_type=jnp.float32).astype(jnp.bfloat16)
    query_h = qkv[:, :own_q].reshape(sequence_count, seq_rows, heads, HEAD_SIZE)
    key_h = jnp.repeat(
        qkv[:, own_q : own_q + own_kv].reshape(sequence_count, seq_rows, kv_heads, HEAD_SIZE),
        group,
        axis=2,
    )
    value_h = jnp.repeat(
        qkv[:, own_q + own_kv :].reshape(sequence_count, seq_rows, kv_heads, HEAD_SIZE),
        group,
        axis=2,
    )
    block_rows = min(512, seq_rows)
    mixed_h, totals, saved_state = attend(query_h, key_h, value_h, block_rows)
    mixed_rows = lax.all_to_all(
        mixed_h.reshape(seq_rows, own_q), "seq", split_axis=0, concat_axis=1, tiled=True
    )
    projected = jnp.einsum("rc,dc->rd", mixed_rows, w_out, preferred_element_type=jnp.float32)
    inverse_one = scale_rows(projected)
    middle = tok_rows + projected * inverse_one * factor[1]
    inverse_two = scale_rows(middle)
    normed_mid = (middle * inverse_two * factor[2]).astype(jnp.bfloat16)
    whole_mlp = lax.all_gather(mlp_weight.astype(jnp.bfloat16), "fsdp", axis=1, tiled=True)
    mlp_parts = (whole_mlp[0], whole_mlp[1], whole_mlp[2])
    chunk_shape = (mlp_chunks, row_count // mlp_chunks, feat_width)
    hidden = whole_mlp.shape[2]
    mlp_rows, hidden_activation, gelu_rows, slope_rows, ffn_out = mlp_half(
        True, n_seq, normed_mid.reshape(chunk_shape), mlp_parts, (), 2
    )
    ffn_out = ffn_out.reshape(row_count, feat_width)
    inverse_three = scale_rows(ffn_out)
    block_out = middle + ffn_out * inverse_three * factor[3]
    dffn, gain_three = norm_back(ffn_out, inverse_three, factor[3], upstream)
    dffn_rows, gate_gradient, up_gradient_half, dnormed_mid = mlp_half(
        False,
        n_seq,
        dffn.astype(jnp.bfloat16).reshape(chunk_shape),
        mlp_parts,
        (gelu_rows, slope_rows),
        3,
    )
    dnormed_mid = dnormed_mid.reshape(row_count, feat_width)
    mlp_rows = mlp_rows.reshape(-1, feat_width)
    dffn_rows = dffn_rows.reshape(-1, feat_width)
    hidden_activation = hidden_activation.reshape(-1, hidden)
    gate_gradient = gate_gradient.reshape(-1, hidden)
    up_gradient_half = up_gradient_half.reshape(-1, hidden)
    grad_gate = jnp.einsum("rd,rf->df", mlp_rows, gate_gradient, preferred_element_type=jnp.float32)
    grad_up = jnp.einsum(
        "rd,rf->df", mlp_rows, up_gradient_half, preferred_element_type=jnp.float32
    )
    grad_down = jnp.einsum(
        "rd,rf->df", dffn_rows, hidden_activation, preferred_element_type=jnp.float32
    )
    mlp_grad = lax.psum_scatter(
        jnp.stack([grad_gate, grad_up, grad_down]).astype(jnp.bfloat16),
        "fsdp",
        scatter_dimension=1,
        tiled=True,
    ).astype(jnp.float32)
    dmid_part, gain_two = norm_back(middle, inverse_two, factor[2], dnormed_mid)
    dmiddle = upstream + dmid_part
    dproj, gain_one = norm_back(projected, inverse_one, factor[1], dmiddle)
    dproj_bf = dproj.astype(jnp.bfloat16)
    dmixed = jnp.dot(dproj_bf, w_out, preferred_element_type=jnp.float32).astype(jnp.bfloat16)
    dmixed_h = lax.all_to_all(dmixed, "seq", split_axis=1, concat_axis=0, tiled=True).reshape(
        sequence_count, seq_rows, heads, HEAD_SIZE
    )
    grad_out = jnp.einsum("tr,tc->rc", dproj_bf, mixed_rows, preferred_element_type=jnp.float32)
    grad_out = lax.psum_scatter(
        grad_out.astype(jnp.bfloat16), AXES, scatter_dimension=0, tiled=True
    ).astype(jnp.float32)
    dquery_h, dkey_h, dvalue_h = attend_back(
        query_h, key_h, value_h, mixed_h, totals, dmixed_h, block_rows
    )

    def group_sum(values):
        return (
            jnp.sum(
                values.astype(jnp.float32).reshape(seq_rows, kv_heads, group, HEAD_SIZE), axis=2
            )
            .astype(jnp.bfloat16)
            .reshape(seq_rows, own_kv)
        )

    dqkv = jnp.concatenate(
        [dquery_h.reshape(seq_rows, own_q), group_sum(dkey_h), group_sum(dvalue_h)], axis=1
    )
    dnormed_in = lax.psum_scatter(
        jnp.einsum("rc,dc->rd", dqkv, w_qkv, preferred_element_type=jnp.float32).astype(
            jnp.bfloat16
        ),
        "seq",
        scatter_dimension=0,
        tiled=True,
    ).astype(jnp.float32)
    grad_qkv = jnp.einsum("tr,tc->rc", whole_xn, dqkv, preferred_element_type=jnp.float32)
    grad_qkv = jnp.transpose(
        grad_qkv.astype(jnp.bfloat16).reshape(n_fsdp, n_seq, n_mlp, share, own_width),
        (0, 2, 1, 3, 4),
    ).reshape(feat_width, own_width)
    grad_qkv = lax.psum_scatter(grad_qkv, ("fsdp", "mlp"), scatter_dimension=0, tiled=True)
    grad_qkv = jnp.transpose(
        lax.all_to_all(
            grad_qkv.reshape(n_seq, share, own_width),
            "seq",
            split_axis=0,
            concat_axis=0,
            tiled=True,
        ),
        (1, 0, 2),
    ).astype(jnp.float32)
    attn_grad = jnp.concatenate(
        [
            grad_qkv[:, :, :own_q].reshape(share, query_total_width),
            grad_qkv[:, :, own_q : own_q + own_kv].reshape(share, key_value_width),
            grad_qkv[:, :, own_q + own_kv :].reshape(share, key_value_width),
            grad_out,
        ],
        axis=1,
    )
    dinput_part, gain_zero = norm_back(tok_rows, inverse_in, factor[0], dnormed_in)
    input_grad = dmiddle + dinput_part

    gain_sums = jnp.stack([gain_zero, gain_one, gain_two, gain_three])
    gain_parts = jnp.transpose(gain_sums.reshape(4, count, feat_width // count), (1, 0, 2))
    gain_parts = jnp.pad(gain_parts, ((0, 0), (0, 4), (0, 128 - feat_width // count)))
    norm_grad = jnp.sum(exchange(sizes, gain_parts, 1), axis=0)[
        : norm_weight.shape[0], : norm_weight.shape[1]
    ]

    attn_new, first_attn_new, second_attn_new = adam_update(
        attention_matrix, attn_grad, attention_first_moment, attention_second_moment, decay_rate
    )
    mlp_new, first_mlp_new, second_mlp_new = adam_update(
        mlp_weight, mlp_grad, first_mlp, second_mlp, decay_rate
    )
    norm_new, first_norm_new, second_norm_new = adam_update(
        norm_weight, norm_grad, first_norm, second_norm, 0.0
    )
    return (
        block_out.reshape(block_in.shape),
        input_grad.reshape(block_in.shape),
        attn_grad,
        attn_new,
        first_attn_new,
        second_attn_new,
        mlp_grad,
        mlp_new,
        first_mlp_new,
        second_mlp_new,
        norm_grad,
        norm_new,
        first_norm_new,
        second_norm_new,
    )


def solution(mesh):
    sizes = (mesh.shape["fsdp"], mesh.shape["seq"], mesh.shape["mlp"])
    fits = KEY_VALUE_HEADS % sizes[1] == 0 and sizes[2] == 2
    body = functools.partial(on_device, sizes) if fits else on_device_generic
    placed = (
        P(("fsdp", "mlp"), "seq", None),
        P(("fsdp", "mlp"), "seq", None),
        P(("fsdp", "seq", "mlp"), None),
        P(("fsdp", "seq", "mlp"), None),
        P(("fsdp", "seq", "mlp"), None),
        P(None, "fsdp", ("seq", "mlp")),
        P(None, "fsdp", ("seq", "mlp")),
        P(None, "fsdp", ("seq", "mlp")),
        P(None, ("fsdp", "seq", "mlp")),
        P(None, ("fsdp", "seq", "mlp")),
        P(None, ("fsdp", "seq", "mlp")),
    )
    return jax.shard_map(
        body,
        mesh=mesh,
        in_specs=placed,
        out_specs=(
            P(("fsdp", "mlp"), "seq", None),
            P(("fsdp", "mlp"), "seq", None),
            P(("fsdp", "seq", "mlp"), None),
            P(("fsdp", "seq", "mlp"), None),
            P(("fsdp", "seq", "mlp"), None),
            P(("fsdp", "seq", "mlp"), None),
            P(None, "fsdp", ("seq", "mlp")),
            P(None, "fsdp", ("seq", "mlp")),
            P(None, "fsdp", ("seq", "mlp")),
            P(None, "fsdp", ("seq", "mlp")),
            P(None, ("fsdp", "seq", "mlp")),
            P(None, ("fsdp", "seq", "mlp")),
            P(None, ("fsdp", "seq", "mlp")),
            P(None, ("fsdp", "seq", "mlp")),
        ),
        check_vma=False,
    )
```

```python
import functools
import math

import jax
import jax.numpy as jnp
from jax import lax
from jax.experimental import pallas as pl
from jax.experimental.pallas import tpu as pltpu
from jax.sharding import PartitionSpec as P

QUERY_HEADS = 8
KEY_VALUE_HEADS = 4
HEAD_SIZE = 256


softcap = 50.0
norm_eps = 1e-06
beta_one = 0.9
beta_two = 0.95
adam_eps = 1e-08
learn_rate = 0.01
decay_rate = 0.1
step_count = 2
gelu_scale = math.sqrt(2.0 / math.pi)
gelu_cubic = 0.044715
mlp_chunks = 4
row_chunks = 2


def scale_rows(values):
    return lax.rsqrt(jnp.mean(values * values, axis=-1, keepdims=True) + norm_eps)


def norm_back(values, inverse, factor, upstream):
    normed = values * inverse
    scaled = upstream * factor
    inner_mean = jnp.mean(scaled * normed, axis=-1, keepdims=True)
    return (inverse * (scaled - normed * inner_mean), jnp.sum(upstream * normed, axis=0))


def gelu_tanh(values):
    return jax.nn.gelu(values, approximate=True)


def adam_update(weight, gradient, first_moment, second_moment, decay_factor):
    first_new = beta_one * first_moment + (1.0 - beta_one) * gradient
    second_new = beta_two * second_moment + (1.0 - beta_two) * gradient * gradient
    first_hat = first_new / (1.0 - beta_one**step_count)
    second_hat = second_new / (1.0 - beta_two**step_count)
    weight_new = weight - learn_rate * (
        first_hat / (jnp.sqrt(second_hat) + adam_eps) + decay_factor * weight
    )
    return (weight_new, first_new, second_new)


def forward_scores(queries, key_head_rows, row_start):
    head_width = queries.shape[3]
    raw_scores = jnp.einsum(
        "sqlc,sklc->slqk", queries, key_head_rows, preferred_element_type=jnp.float32
    ) * head_width ** (-0.5)
    capped = softcap * jnp.tanh(raw_scores / softcap)
    shape_pair = (queries.shape[1], key_head_rows.shape[1])
    row_index = row_start + lax.broadcasted_iota(jnp.int32, shape_pair, 0)
    col_index = lax.broadcasted_iota(jnp.int32, shape_pair, 1)
    return (capped, col_index <= row_index)


def attend(queries, key_head_rows, value_head_rows, block_rows):
    sequence_count, length, head_count, head_width = queries.shape

    def one_block(block_index, carry_state):
        row_start = block_index * block_rows
        query_part = lax.dynamic_slice_in_dim(queries, row_start, block_rows, 1)
        capped, causal = forward_scores(query_part, key_head_rows, row_start)
        logsum = jnp.log(jnp.sum(jnp.where(causal, jnp.exp(capped), 0.0), axis=-1))
        prob_full = jnp.where(causal, jnp.exp(capped - logsum[..., None]), 0.0)
        prob_bf = prob_full.astype(jnp.bfloat16)
        mixed_part = jnp.einsum(
            "slqk,sklc->sqlc", prob_bf, value_head_rows, preferred_element_type=jnp.float32
        ).astype(jnp.bfloat16)
        outputs = lax.dynamic_update_slice_in_dim(carry_state[0], mixed_part, row_start, 1)
        totals = lax.dynamic_update_slice_in_dim(carry_state[1], logsum, row_start, 2)
        return (outputs, totals)

    start_state = (
        jnp.zeros(queries.shape, jnp.bfloat16),
        jnp.zeros((sequence_count, head_count, length), jnp.float32),
    )
    end_state = lax.fori_loop(0, length // block_rows, one_block, start_state)
    return (end_state[0], end_state[1], tuple(end_state[2:]))


def attend_back(queries, key_head_rows, value_head_rows, outputs, totals, upstream, block_rows):
    sequence_count, length, head_count, head_width = queries.shape
    row_inner = jnp.sum(upstream.astype(jnp.float32) * outputs.astype(jnp.float32), axis=-1)

    def one_block(block_index, carry_state):
        dquery, dkey_acc, dvalue_acc = carry_state
        row_start = block_index * block_rows
        query_part = lax.dynamic_slice_in_dim(queries, row_start, block_rows, 1)
        grad_part = lax.dynamic_slice_in_dim(upstream, row_start, block_rows, 1)
        inner_part = lax.dynamic_slice_in_dim(row_inner, row_start, block_rows, 1)
        logsum = lax.dynamic_slice_in_dim(totals, row_start, block_rows, 2)
        capped, causal = forward_scores(query_part, key_head_rows, row_start)
        prob_full = jnp.where(causal, jnp.exp(capped - logsum[..., None]), 0.0)
        dprob = jnp.einsum(
            "sqlc,sklc->slqk", grad_part, value_head_rows, preferred_element_type=jnp.float32
        )
        dcapped = prob_full * (dprob - jnp.transpose(inner_part, (0, 2, 1))[..., None])
        dscore = (
            dcapped * (1.0 - capped / softcap * (capped / softcap)) * head_width ** (-0.5)
        ).astype(jnp.bfloat16)
        dquery_part = jnp.einsum(
            "slqk,sklc->sqlc", dscore, key_head_rows, preferred_element_type=jnp.float32
        ).astype(jnp.bfloat16)
        dquery = lax.dynamic_update_slice_in_dim(dquery, dquery_part, row_start, 1)
        dkey_acc = dkey_acc + jnp.einsum(
            "slqk,sqlc->sklc", dscore, query_part, preferred_element_type=jnp.float32
        )
        dvalue_acc = dvalue_acc + jnp.einsum(
            "slqk,sqlc->sklc",
            prob_full.astype(jnp.bfloat16),
            grad_part,
            preferred_element_type=jnp.float32,
        )
        return (dquery, dkey_acc, dvalue_acc)

    start_state = (
        jnp.zeros(queries.shape, jnp.bfloat16),
        jnp.zeros(key_head_rows.shape, jnp.float32),
        jnp.zeros(value_head_rows.shape, jnp.float32),
    )
    dquery, dkey_acc, dvalue_acc = lax.fori_loop(0, length // block_rows, one_block, start_state)
    return (dquery, dkey_acc.astype(jnp.bfloat16), dvalue_acc.astype(jnp.bfloat16))


def on_device_generic(
    block_in,
    cotangent,
    attention_matrix,
    attention_first_moment,
    attention_second_moment,
    mlp_weight,
    first_mlp,
    second_mlp,
    norm_weight,
    first_norm,
    second_norm,
):
    sequence_count, token_length, feat_width = block_in.shape
    row_count = sequence_count * token_length
    query_total_width = QUERY_HEADS * HEAD_SIZE
    key_value_width = KEY_VALUE_HEADS * HEAD_SIZE
    query_group_count = QUERY_HEADS // KEY_VALUE_HEADS
    whole_attn, gain_rows = (
        lax.all_gather(
            attention_matrix.astype(jnp.bfloat16), ("fsdp", "seq", "mlp"), axis=0, tiled=True
        ),
        lax.all_gather(
            norm_weight.astype(jnp.bfloat16), ("fsdp", "seq", "mlp"), axis=1, tiled=True
        ),
    )
    factor = 1.0 + gain_rows.astype(jnp.float32)
    w_qkv = whole_attn[:, : query_total_width + 2 * key_value_width]
    w_out = whole_attn[:, query_total_width + 2 * key_value_width :]
    tok_rows = block_in.reshape(row_count, feat_width)
    upstream = cotangent.reshape(row_count, feat_width)
    inverse_in = scale_rows(tok_rows)
    normed_in = (tok_rows * inverse_in * factor[0]).astype(jnp.bfloat16)
    query_key_value_rows = jnp.dot(normed_in, w_qkv, preferred_element_type=jnp.float32).astype(
        jnp.bfloat16
    )
    queries = query_key_value_rows[:, :query_total_width].reshape(
        sequence_count, token_length, QUERY_HEADS, HEAD_SIZE
    )
    key_head_rows = jnp.repeat(
        query_key_value_rows[:, query_total_width : query_total_width + key_value_width].reshape(
            sequence_count, token_length, KEY_VALUE_HEADS, HEAD_SIZE
        ),
        query_group_count,
        axis=2,
    )
    value_head_rows = jnp.repeat(
        query_key_value_rows[:, query_total_width + key_value_width :].reshape(
            sequence_count, token_length, KEY_VALUE_HEADS, HEAD_SIZE
        ),
        query_group_count,
        axis=2,
    )
    query_h, key_h, value_h = (
        lax.all_to_all(queries, "seq", split_axis=2, concat_axis=1, tiled=True),
        lax.all_to_all(key_head_rows, "seq", split_axis=2, concat_axis=1, tiled=True),
        lax.all_to_all(value_head_rows, "seq", split_axis=2, concat_axis=1, tiled=True),
    )
    block_rows = min(512, query_h.shape[1])
    mixed_h, totals, saved_state = attend(query_h, key_h, value_h, block_rows)
    mixed = lax.all_to_all(mixed_h, "seq", split_axis=1, concat_axis=2, tiled=True)
    mixed_rows = mixed.reshape(row_count, query_total_width)
    projected = jnp.einsum("rc,dc->rd", mixed_rows, w_out, preferred_element_type=jnp.float32)
    inverse_one = scale_rows(projected)
    middle = tok_rows + projected * inverse_one * factor[1]
    inverse_two = scale_rows(middle)
    normed_mid = (middle * inverse_two * factor[2]).astype(jnp.bfloat16)
    mlp_rows = lax.all_gather(normed_mid, ("seq", "mlp"), axis=0, tiled=True)
    whole_mlp = lax.all_gather(mlp_weight.astype(jnp.bfloat16), "fsdp", axis=1, tiled=True)
    gate_pre = jnp.dot(mlp_rows, whole_mlp[0], preferred_element_type=jnp.float32)
    up_pre = jnp.dot(mlp_rows, whole_mlp[1], preferred_element_type=jnp.float32)
    activated, gelu_back = jax.vjp(gelu_tanh, gate_pre)
    hidden_activation = (activated * up_pre).astype(jnp.bfloat16)
    ffn_part = jnp.einsum(
        "rf,df->rd", hidden_activation, whole_mlp[2], preferred_element_type=jnp.float32
    )
    ffn_out = lax.psum_scatter(
        ffn_part.astype(jnp.bfloat16), ("seq", "mlp"), scatter_dimension=0, tiled=True
    ).astype(jnp.float32)
    inverse_three = scale_rows(ffn_out)
    block_out = middle + ffn_out * inverse_three * factor[3]
    dffn, gain_three = norm_back(ffn_out, inverse_three, factor[3], upstream)
    dffn_rows = lax.all_gather(dffn.astype(jnp.bfloat16), ("seq", "mlp"), axis=0, tiled=True)
    dhidden = jnp.dot(dffn_rows, whole_mlp[2], preferred_element_type=jnp.float32)
    grad_down = jnp.einsum(
        "rd,rf->df", dffn_rows, hidden_activation, preferred_element_type=jnp.float32
    )
    gate_gradient = gelu_back(dhidden * up_pre)[0].astype(jnp.bfloat16)
    up_gradient_half = (dhidden * activated).astype(jnp.bfloat16)
    grad_gate = jnp.einsum("rd,rf->df", mlp_rows, gate_gradient, preferred_element_type=jnp.float32)
    grad_up = jnp.einsum(
        "rd,rf->df", mlp_rows, up_gradient_half, preferred_element_type=jnp.float32
    )
    dnormed_part = jnp.einsum(
        "rf,df->rd", gate_gradient, whole_mlp[0], preferred_element_type=jnp.float32
    ) + jnp.einsum("rf,df->rd", up_gradient_half, whole_mlp[1], preferred_element_type=jnp.float32)
    mlp_grad = lax.psum_scatter(
        jnp.stack([grad_gate, grad_up, grad_down]).astype(jnp.bfloat16),
        "fsdp",
        scatter_dimension=1,
        tiled=True,
    ).astype(jnp.float32)
    dnormed_mid = lax.psum_scatter(
        dnormed_part.astype(jnp.bfloat16), ("seq", "mlp"), scatter_dimension=0, tiled=True
    ).astype(jnp.float32)
    dmid_part, gain_two = norm_back(middle, inverse_two, factor[2], dnormed_mid)
    dmiddle = upstream + dmid_part
    dproj, gain_one = norm_back(projected, inverse_one, factor[1], dmiddle)
    dproj_bf = dproj.astype(jnp.bfloat16)
    dmixed = jnp.dot(dproj_bf, w_out, preferred_element_type=jnp.float32).astype(jnp.bfloat16)
    dmixed_h = lax.all_to_all(
        dmixed.reshape(sequence_count, token_length, QUERY_HEADS, HEAD_SIZE),
        "seq",
        split_axis=2,
        concat_axis=1,
        tiled=True,
    )
    dquery_h, dkey_h, dvalue_h = attend_back(
        query_h, key_h, value_h, mixed_h, totals, dmixed_h, block_rows
    )
    dquery, key_gradient_single, value_gradient_single = (
        lax.all_to_all(dquery_h, "seq", split_axis=1, concat_axis=2, tiled=True),
        lax.all_to_all(dkey_h, "seq", split_axis=1, concat_axis=2, tiled=True),
        lax.all_to_all(dvalue_h, "seq", split_axis=1, concat_axis=2, tiled=True),
    )
    key_gradient = jnp.sum(
        key_gradient_single.astype(jnp.float32).reshape(
            sequence_count, token_length, KEY_VALUE_HEADS, query_group_count, HEAD_SIZE
        ),
        axis=3,
    ).astype(jnp.bfloat16)
    value_gradient = jnp.sum(
        value_gradient_single.astype(jnp.float32).reshape(
            sequence_count, token_length, KEY_VALUE_HEADS, query_group_count, HEAD_SIZE
        ),
        axis=3,
    ).astype(jnp.bfloat16)
    dqkv = jnp.concatenate(
        [
            dquery.reshape(row_count, query_total_width),
            key_gradient.reshape(row_count, key_value_width),
            value_gradient.reshape(row_count, key_value_width),
        ],
        axis=1,
    )
    dnormed_in = jnp.einsum("rc,dc->rd", dqkv, w_qkv, preferred_element_type=jnp.float32)
    dinput_part, gain_zero = norm_back(tok_rows, inverse_in, factor[0], dnormed_in)
    input_grad = dmiddle + dinput_part
    fsdp_count = lax.axis_size("fsdp")
    seq_count = lax.axis_size("seq")
    mlp_count = lax.axis_size("mlp")
    seq_index = lax.axis_index("seq")
    row_share = feat_width // (fsdp_count * seq_count * mlp_count)
    whole_xn, whole_dqkv, whole_dproj, whole_mixed = (
        lax.all_gather(normed_in, "seq", axis=0, tiled=True),
        lax.all_gather(dqkv, "seq", axis=0, tiled=True),
        lax.all_gather(dproj_bf, "seq", axis=0, tiled=True),
        lax.all_gather(mixed_rows, "seq", axis=0, tiled=True),
    )

    def own_columns(values):
        parted = values.reshape(values.shape[0], fsdp_count, seq_count, mlp_count, row_share)
        picked = lax.dynamic_index_in_dim(parted, seq_index, 2, keepdims=False)
        return picked.reshape(values.shape[0], fsdp_count * mlp_count * row_share)

    xn_own = own_columns(whole_xn)
    dproj_own = own_columns(whole_dproj)
    grad_rows = jnp.concatenate(
        [
            jnp.einsum("tr,tc->rc", xn_own, whole_dqkv, preferred_element_type=jnp.float32),
            jnp.einsum("tr,tc->rc", dproj_own, whole_mixed, preferred_element_type=jnp.float32),
        ],
        axis=1,
    )
    attn_grad = lax.psum_scatter(
        grad_rows.astype(jnp.bfloat16), ("fsdp", "mlp"), scatter_dimension=0, tiled=True
    ).astype(jnp.float32)
    norm_grad = lax.psum_scatter(
        jnp.stack([gain_zero, gain_one, gain_two, gain_three]),
        ("fsdp", "seq", "mlp"),
        scatter_dimension=1,
        tiled=True,
    )
    attn_new, first_attn_new, second_attn_new = adam_update(
        attention_matrix, attn_grad, attention_first_moment, attention_second_moment, decay_rate
    )
    mlp_new, first_mlp_new, second_mlp_new = adam_update(
        mlp_weight, mlp_grad, first_mlp, second_mlp, decay_rate
    )
    norm_new, first_norm_new, second_norm_new = adam_update(
        norm_weight, norm_grad, first_norm, second_norm, 0.0
    )
    return (
        block_out.reshape(block_in.shape),
        input_grad.reshape(block_in.shape),
        attn_grad,
        attn_new,
        first_attn_new,
        second_attn_new,
        mlp_grad,
        mlp_new,
        first_mlp_new,
        second_mlp_new,
        norm_grad,
        norm_new,
        first_norm_new,
        second_norm_new,
    )


MESH = pl.DeviceIdType.MESH
AXES = ("fsdp", "seq", "mlp")


def exchange_kernel(
    sizes,
    mine_ref,
    block_ref,
    out_ref,
    landed_ref,
    send_sem,
    recv_sem,
    block_send,
    block_recv,
):
    n_fsdp, n_seq, n_mlp = sizes
    count = n_fsdp * n_seq * n_mlp
    fsdp, at, core = lax.axis_index("fsdp"), lax.axis_index("seq"), lax.axis_index("mlp")
    me = (fsdp * n_seq + at) * n_mlp + core
    slots = mine_ref.shape[0]

    def place(index):
        return (index // (n_seq * n_mlp), (index // n_mlp) % n_seq, index % n_mlp)

    barrier = pltpu.get_barrier_semaphore()

    @pl.loop(1, count)
    def _(step):
        pl.semaphore_signal(barrier, inc=1, device_id=place((me + step) % count), device_id_type=MESH)

    pl.semaphore_wait(barrier, count - 1)

    def block_to(step):
        to = lax.rem(at + step, n_seq)
        return pltpu.make_async_remote_copy(
            src_ref=block_ref.at[to],
            dst_ref=landed_ref.at[at],
            send_sem=block_send.at[step],
            recv_sem=block_recv.at[step],
            device_id=(fsdp, to, core),
            device_id_type=MESH,
        )

    def copy_to(step):
        to = (me + step) % count
        return pltpu.make_async_remote_copy(
            src_ref=mine_ref.at[to % slots],
            dst_ref=out_ref.at[me],
            send_sem=send_sem.at[step],
            recv_sem=recv_sem.at[step],
            device_id=place(to),
            device_id_type=MESH,
        )

    @pl.loop(1, count)
    def _(step):
        copy_to(step).start()

    for step in range(1, n_seq):
        block_to(step).start()
    own = pltpu.make_async_copy(block_ref.at[at], landed_ref.at[at], block_send.at[0])
    own.start()
    out_ref[pl.ds(me, 1)] = mine_ref[pl.ds(me % slots, 1)]

    @pl.loop(1, count)
    def _(step):
        copy_to(step).wait()

    for step in range(1, n_seq):
        block_to(step).wait()
    own.wait()


def exchange(sizes, mine, blocks, collective_id):
    count = sizes[0] * sizes[1] * sizes[2]
    vmem = pl.BlockSpec(memory_space=pltpu.VMEM)
    return pl.pallas_call(
        functools.partial(exchange_kernel, sizes),
        name="exchange",
        out_shape=[
            jax.ShapeDtypeStruct((count,) + mine.shape[1:], mine.dtype),
            jax.ShapeDtypeStruct(blocks.shape, blocks.dtype),
        ],
        in_specs=[vmem, vmem],
        out_specs=[vmem, vmem],
        scratch_shapes=[
            pltpu.SemaphoreType.DMA((count,)),
            pltpu.SemaphoreType.DMA((count,)),
            pltpu.SemaphoreType.DMA((sizes[1],)),
            pltpu.SemaphoreType.DMA((sizes[1],)),
        ],
        compiler_params=pltpu.CompilerParams(collective_id=collective_id, has_side_effects=True),
    )(mine, blocks)


def neighbour_barrier(seq_count, at, up, down, sibling):
    barrier = pltpu.get_barrier_semaphore()

    @pl.when(at < seq_count - 1)
    def _():
        pl.semaphore_signal(barrier, inc=1, device_id=up, device_id_type=MESH)

    @pl.when(at > 0)
    def _():
        pl.semaphore_signal(barrier, inc=1, device_id=down, device_id_type=MESH)

    peers = jnp.where(at < seq_count - 1, 1, 0) + jnp.where(at > 0, 1, 0)
    if sibling is not None:
        pl.semaphore_signal(barrier, inc=1, device_id=sibling, device_id_type=MESH)
        peers = peers + 1
    pl.semaphore_wait(barrier, peers)


class RowGather:
    def __init__(self, n, own, whole, send_sem, recv_sem, pair=True):
        self.n, self.own, self.whole, self.pair = n, own, whole, pair
        self.send_sem, self.recv_sem = send_sem, recv_sem
        self.fsdp, self.at, self.core = (
            lax.axis_index("fsdp"),
            lax.axis_index("seq"),
            lax.axis_index("mlp"),
        )
        self.up = (self.fsdp, lax.rem(self.at + 1, n), self.core)
        self.down = (self.fsdp, lax.rem(self.at + n - 1, n), self.core)
        self.sibling = (self.fsdp, self.at, 1 - self.core)
        self.base = self.core * n if pair else 0

    def spot(self, chunk, slot):
        return self.whole.at[chunk, slot] if self.pair else self.whole.at[slot, chunk]

    def copy(self, chunk, block, way, own=False):
        slot = self.base + block
        return pltpu.make_async_remote_copy(
            src_ref=self.own.at[chunk] if own else self.spot(chunk, slot),
            dst_ref=self.spot(chunk, slot),
            send_sem=self.send_sem.at[chunk, way, block],
            recv_sem=self.recv_sem.at[chunk, slot],
            device_id=(self.up, self.down, self.sibling)[way],
            device_id_type=MESH,
        )

    def arrival(self, chunk, slot):
        return pltpu.make_async_remote_copy(
            src_ref=self.own.at[chunk],
            dst_ref=self.spot(chunk, slot),
            send_sem=self.send_sem.at[chunk, 0, 0],
            recv_sem=self.recv_sem.at[chunk, slot],
            device_id=self.sibling if self.pair else self.up,
            device_id_type=MESH,
        )

    def begin(self, chunk):
        @pl.when(self.at < self.n - 1)
        def _():
            self.copy(chunk, self.at, 0, True).start()

        @pl.when(self.at > 0)
        def _():
            self.copy(chunk, self.at, 1, True).start()

        if self.pair:
            self.copy(chunk, self.at, 2, True).start()

    def step(self, chunk, hop):
        below, above = self.at - hop, self.at + hop

        @pl.when(below >= 0)
        def _():
            self.arrival(chunk, self.base + below).wait_recv()

            @pl.when(self.at < self.n - 1)
            def _():
                self.copy(chunk, below, 0).start()

            if self.pair:
                self.copy(chunk, below, 2).start()

        @pl.when(above < self.n)
        def _():
            self.arrival(chunk, self.base + above).wait_recv()

            @pl.when(self.at > 0)
            def _():
                self.copy(chunk, above, 1).start()

            if self.pair:
                self.copy(chunk, above, 2).start()

    def finish(self, chunk):
        for block in range(self.n):
            self.arrival(chunk, (1 - self.core) * self.n + block).wait_recv()

    def drain(self, chunk):
        for block in range(self.n):

            @pl.when((block <= self.at) & (self.at < self.n - 1))
            def _():
                self.copy(chunk, block, 0).wait_send()

            @pl.when((block >= self.at) & (self.at > 0))
            def _():
                self.copy(chunk, block, 1).wait_send()

            if self.pair:
                self.copy(chunk, block, 2).wait_send()


class RowScatter:
    def __init__(self, n, total, held, send_sem, recv_sem):
        self.n, self.total, self.held = n, total, held
        self.send_sem, self.recv_sem = send_sem, recv_sem
        self.fsdp, self.at, self.core = (
            lax.axis_index("fsdp"),
            lax.axis_index("seq"),
            lax.axis_index("mlp"),
        )
        self.up = (self.fsdp, lax.rem(self.at + 1, n), self.core)
        self.down = (self.fsdp, lax.rem(self.at + n - 1, n), self.core)

    def copy(self, chunk, block, way):
        slot = block
        if way == 1:
            slot = jnp.where(block == self.at - 1, self.n, block)
        return pltpu.make_async_remote_copy(
            src_ref=self.total.at[chunk, block],
            dst_ref=self.held.at[chunk, slot],
            send_sem=self.send_sem.at[chunk, way, block],
            recv_sem=self.recv_sem.at[chunk, slot],
            device_id=(self.up, self.down)[way],
            device_id_type=MESH,
        )

    def arrive(self, chunk, slot):
        pltpu.make_async_remote_copy(
            src_ref=self.total.at[chunk, 0],
            dst_ref=self.held.at[chunk, slot],
            send_sem=self.send_sem.at[chunk, 0, 0],
            recv_sem=self.recv_sem.at[chunk, slot],
            device_id=self.up,
            device_id_type=MESH,
        ).wait_recv()

    def add(self, chunk, block):
        self.arrive(chunk, block)
        self.total[chunk, block] = (
            self.total[chunk, block].astype(jnp.float32)
            + self.held[chunk, block].astype(jnp.float32)
        ).astype(jnp.bfloat16)

    def step(self, chunk, wave):
        far = self.n - 1 - self.at

        @pl.when(self.at < wave)
        def _():
            block = self.n - wave + self.at

            @pl.when(self.at > 0)
            def _():
                self.add(chunk, block)

            self.copy(chunk, block, 0).start()

        @pl.when(far < wave)
        def _():
            block = wave - 1 - far

            @pl.when(far > 0)
            def _():
                self.add(chunk, block)

            self.copy(chunk, block, 1).start()

    def finish(self, chunk, store):
        own = self.total[chunk, self.at].astype(jnp.float32)
        last = self.n - 1

        @pl.when(self.at == 0)
        def _():
            self.arrive(chunk, self.n)
            store(own + self.held[chunk, self.n].astype(jnp.float32))

        @pl.when(self.at == last)
        def _():
            self.arrive(chunk, self.at)
            store(own + self.held[chunk, self.at].astype(jnp.float32))

        @pl.when((self.at > 0) & (self.at < last))
        def _():
            self.arrive(chunk, self.at)
            self.arrive(chunk, self.n)
            store(
                own
                + self.held[chunk, self.at].astype(jnp.float32)
                + self.held[chunk, self.n].astype(jnp.float32)
            )

    def drain(self, chunk):
        for block in range(self.n):

            @pl.when(block > self.at)
            def _():
                self.copy(chunk, block, 0).wait_send()

            @pl.when(block < self.at)
            def _():
                self.copy(chunk, block, 1).wait_send()


def column_tiles(width, tile):
    return [(start, min(tile, width - start)) for start in range(0, width, tile)]


def mlp_kernel(
    forward,
    n,
    own,
    weights,
    saved_in,
    whole_out,
    saved_out,
    result,
    whole,
    w_vmem,
    loaded,
    stored,
    partner,
    arrived,
    total,
    held,
    gather_send,
    gather_recv,
    pair_send,
    pair_recv,
    scatter_send,
    scatter_recv,
    own_sem,
    w_sem,
    load_sem,
    store_sem,
    whole_sem,
):
    chunks, rows, width = own.shape
    hidden = w_vmem[0].shape[1]
    line_rows = n * rows
    all_rows = 2 * line_rows
    gather = RowGather(n, own, whole, gather_send, gather_recv)
    scatter = RowScatter(n, total, held, scatter_send, scatter_recv)
    core = gather.core

    w_copies = [
        pltpu.make_async_copy(w, v, w_sem.at[i]) for i, (w, v) in enumerate(zip(weights, w_vmem))
    ]
    for copy in w_copies:
        copy.start()
    neighbour_barrier(n, gather.at, gather.up, gather.down, gather.sibling)
    gather.begin(0)
    own_copies = [
        pltpu.make_async_copy(own.at[c], whole.at[c, core * n + gather.at], own_sem.at[c])
        for c in range(chunks)
    ]
    for copy in own_copies:
        copy.start()

    def load(chunk, slot):
        return [
            pltpu.make_async_copy(ref.at[chunk], buf.at[slot], load_sem.at[i, slot])
            for i, (ref, buf) in enumerate(zip(saved_in, loaded))
        ]

    def store(chunk, slot):
        return [
            pltpu.make_async_copy(buf.at[slot], ref.at[chunk], store_sem.at[i, slot])
            for i, (ref, buf) in enumerate(zip(saved_out, stored))
        ]

    def keep(chunk):
        return pltpu.make_async_copy(whole.at[chunk], whole_out.at[chunk], whole_sem.at[chunk])

    def swap(chunk, slot):
        return pltpu.make_async_remote_copy(
            src_ref=partner.at[slot],
            dst_ref=arrived.at[chunk],
            send_sem=pair_send.at[slot],
            recv_sem=pair_recv.at[chunk],
            device_id=gather.sibling,
            device_id_type=MESH,
        )

    for copy in load(0, 0):
        copy.start()
    for hop in range(1, n):
        gather.step(0, hop)
    for copy in own_copies + w_copies:
        copy.wait()
    gather.finish(0)

    def pair_sum(chunk):
        swap(chunk, 0).wait_recv()
        for block in range(n):
            total[chunk, block] = (
                total[chunk, block].astype(jnp.float32)
                + arrived[chunk, block].astype(jnp.float32)
            ).astype(jnp.bfloat16)

    def finish_chunk(chunk):
        def write(value):
            result[chunk] = value

        scatter.finish(chunk, write)

    tiles = column_tiles(hidden, 256)
    groups = [tiles[: len(tiles) // 2], tiles[len(tiles) // 2 :]]

    @pl.loop(0, chunks)
    def _(chunk):
        slot = lax.rem(chunk, 2)
        more = chunk + 1 < chunks
        behind = chunk > 0

        keep(chunk).start()
        for copy in load(chunk, slot):
            copy.wait()

        @pl.when(more)
        def _():
            gather.begin(chunk + 1)
            for copy in load(chunk + 1, 1 - slot):
                copy.start()

        @pl.when(chunk > 1)
        def _():
            for copy in store(chunk, slot):
                copy.wait()

        def first_half(part):
            for start, size in groups[part]:
                cols = slice(start, start + size)
                tokens = whole[chunk].reshape(all_rows, width)
                if forward:
                    gate = jnp.dot(tokens, w_vmem[0][:, cols], preferred_element_type=jnp.float32)
                    up = jnp.dot(tokens, w_vmem[1][:, cols], preferred_element_type=jnp.float32)
                    inner = gelu_scale * (gate + gelu_cubic * gate * gate * gate)
                    wave = jnp.tanh(inner)
                    half = 0.5 * (1.0 + wave)
                    gelu = gate * half
                    slope = half + 0.5 * gate * (1.0 - wave * wave) * gelu_scale * (
                        1.0 + 3.0 * gelu_cubic * gate * gate
                    )
                    stored[0][slot, :, cols] = (gelu * up).astype(jnp.bfloat16)
                    stored[1][slot, :, cols] = gelu.astype(jnp.bfloat16)
                    stored[2][slot, :, cols] = (slope * up).astype(jnp.bfloat16)
                else:
                    dact = jnp.dot(tokens, w_vmem[2][:, cols], preferred_element_type=jnp.float32)
                    stored[0][slot, :, cols] = (
                        dact * loaded[1][slot, :, cols].astype(jnp.float32)
                    ).astype(jnp.bfloat16)
                    stored[1][slot, :, cols] = (
                        dact * loaded[0][slot, :, cols].astype(jnp.float32)
                    ).astype(jnp.bfloat16)

        def second_half(line, put):
            part = pl.ds(pl.multiple_of(line * line_rows, line_rows), line_rows)
            for start, size in column_tiles(width, 768):
                cols = slice(start, start + size)

                def back(left, right):
                    return lax.dot_general(
                        left[slot, part, :],
                        right[cols, :],
                        (((1,), (1,)), ((), ())),
                        preferred_element_type=jnp.float32,
                    )

                if forward:
                    value = back(stored[0], w_vmem[2])
                else:
                    value = back(stored[0], w_vmem[0]) + back(stored[1], w_vmem[1])
                put(cols, value.astype(jnp.bfloat16).reshape(n, rows, size))

        def between(step):
            @pl.when(more)
            def _():
                if step < n:
                    gather.step(chunk + 1, step)
                else:
                    gather.finish(chunk + 1)

            @pl.when(behind)
            def _():
                if step < n:
                    scatter.step(chunk - 1, step)
                else:
                    finish_chunk(chunk - 1)

        @pl.when(behind)
        def _():
            pair_sum(chunk - 1)

        waits = list(range(1, n + 1))
        first_half(0)
        between(waits.pop(0))
        first_half(1)
        for copy in store(chunk, slot):
            copy.start()
        if len(waits) > 1:
            between(waits.pop(0))

        @pl.when(chunk > 1)
        def _():
            swap(chunk, slot).wait_send()

        def put_partner(cols, value):
            partner[slot, :, :, cols] = value

        second_half(1 - core, put_partner)
        while len(waits) > 1:
            between(waits.pop(0))
        swap(chunk, slot).start()

        def put_total(cols, value):
            total[chunk, :, :, cols] = value

        second_half(core, put_total)
        between(waits.pop(0))

    last = chunks - 1
    pair_sum(last)
    for wave in range(1, n):
        scatter.step(last, wave)
    finish_chunk(last)

    for chunk in range(chunks):
        gather.drain(chunk)
        scatter.drain(chunk)
        keep(chunk).wait()
    for chunk in range(max(chunks - 2, 0), chunks):
        swap(chunk, chunk % 2).wait_send()
        for copy in store(chunk, chunk % 2):
            copy.wait()


def mlp_half(forward, n, own, weights, saved, collective_id):
    chunks, rows, width = own.shape
    hidden = weights[0].shape[1]
    all_rows = 2 * n * rows
    outs = 3 if forward else 2
    hidden_shape = jax.ShapeDtypeStruct((chunks, all_rows, hidden), jnp.bfloat16)

    def kernel(*refs):
        refs = list(refs)

        def take(count):
            taken = refs[:count]
            del refs[:count]
            return taken

        (own_ref,) = take(1)
        weight_refs = take(3)
        saved_refs = take(len(saved))
        (whole_out,) = take(1)
        saved_out = take(outs)
        (result,) = take(1)
        (whole,) = take(1)
        w_vmem = take(3)
        loaded = take(len(saved))
        stored = take(outs)
        mlp_kernel(
            forward,
            n,
            own_ref,
            weight_refs,
            saved_refs,
            whole_out,
            saved_out,
            result,
            whole,
            w_vmem,
            loaded,
            stored,
            *refs,
        )

    hbm = pl.BlockSpec(memory_space=pl.ANY)
    vmem = pl.BlockSpec(memory_space=pltpu.VMEM)
    bf16 = jnp.bfloat16
    flops = 2 * chunks * all_rows * width * hidden * 3
    return pl.pallas_call(
        kernel,
        name="mlp_forward" if forward else "mlp_backward",
        out_shape=(
            [jax.ShapeDtypeStruct((chunks, 2 * n, rows, width), bf16)]
            + [hidden_shape] * outs
            + [jax.ShapeDtypeStruct((chunks, rows, width), jnp.float32)]
        ),
        in_specs=[vmem] + [hbm] * (3 + len(saved)),
        out_specs=[hbm] * (1 + outs) + [vmem],
        scratch_shapes=(
            [pltpu.VMEM((chunks, 2 * n, rows, width), bf16)]
            + [pltpu.VMEM((width, hidden), bf16)] * 3
            + [pltpu.VMEM((2, all_rows, hidden), bf16)] * (len(saved) + outs)
            + [
                pltpu.VMEM((2, n, rows, width), bf16),
                pltpu.VMEM((chunks, n, rows, width), bf16),
                pltpu.VMEM((chunks, n, rows, width), bf16),
                pltpu.VMEM((chunks, n + 1, rows, width), bf16),
                pltpu.SemaphoreType.DMA((chunks, 3, n)),
                pltpu.SemaphoreType.DMA((chunks, 2 * n)),
                pltpu.SemaphoreType.DMA((2,)),
                pltpu.SemaphoreType.DMA((chunks,)),
                pltpu.SemaphoreType.DMA((chunks, 2, n)),
                pltpu.SemaphoreType.DMA((chunks, n + 1)),
                pltpu.SemaphoreType.DMA((chunks,)),
                pltpu.SemaphoreType.DMA((3,)),
                pltpu.SemaphoreType.DMA((max(len(saved), 1), 2)),
                pltpu.SemaphoreType.DMA((outs, 2)),
                pltpu.SemaphoreType.DMA((chunks,)),
            ]
        ),
        compiler_params=pltpu.CompilerParams(
            collective_id=collective_id, has_side_effects=True, vmem_limit_bytes=60 << 20
        ),
        cost_estimate=pl.CostEstimate(
            flops=flops, bytes_accessed=2 * 3 * width * hidden, transcendentals=0
        ),
    )(own, *weights, *saved)


def gather_kernel(n, own, whole, send_sem, recv_sem, own_sem):
    chunks = own.shape[0]
    gather = RowGather(n, own, whole, send_sem, recv_sem, pair=False)
    neighbour_barrier(n, gather.at, gather.up, gather.down, None)
    for chunk in range(chunks):
        gather.begin(chunk)
    own_copies = [
        pltpu.make_async_copy(own.at[c], gather.spot(c, gather.at), own_sem.at[c])
        for c in range(chunks)
    ]
    for copy in own_copies:
        copy.start()
    for hop in range(1, n):
        for chunk in range(chunks):
            gather.step(chunk, hop)
    for copy in own_copies:
        copy.wait()
    for chunk in range(chunks):
        gather.drain(chunk)


def gather_rows(n, own, collective_id):
    chunks = own.shape[0]
    vmem = pl.BlockSpec(memory_space=pltpu.VMEM)
    return pl.pallas_call(
        functools.partial(gather_kernel, n),
        name="gather_rows",
        out_shape=jax.ShapeDtypeStruct((n,) + own.shape, own.dtype),
        in_specs=[vmem],
        out_specs=vmem,
        scratch_shapes=[
            pltpu.SemaphoreType.DMA((chunks, 3, n)),
            pltpu.SemaphoreType.DMA((chunks, n)),
            pltpu.SemaphoreType.DMA((chunks,)),
        ],
        compiler_params=pltpu.CompilerParams(collective_id=collective_id, has_side_effects=True),
    )(own)


def multiply_scatter_kernel(
    n, first, left, right, result, total, held, right_vmem, send_sem, recv_sem, right_sem
):
    chunks, rows, width = result.shape
    depth = left.shape[3]
    scatter = RowScatter(n, total, held, send_sem, recv_sem)
    at, far = scatter.at, n - 1 - scatter.at
    fetch = pltpu.make_async_copy(right, right_vmem, right_sem.at[0])
    fetch.start()
    neighbour_barrier(n, at, scatter.up, scatter.down, None)
    fetch.wait()

    def product(block, chunk, put):
        for start, size in column_tiles(width, 768):
            put(
                slice(start, start + size),
                lax.dot_general(
                    left[block, chunk],
                    right_vmem[start : start + size, first : first + depth],
                    (((1,), (1,)), ((), ())),
                    preferred_element_type=jnp.float32,
                ),
            )

    def send(block, chunk, way, started):
        def put(cols, value):
            total[chunk, block, :, cols] = value.astype(jnp.bfloat16)

        product(block, chunk, put)

        @pl.when(started)
        def _():
            scatter.add(chunk, block)

        scatter.copy(chunk, block, way).start()

    @pl.loop(1, n)
    def _(wave):
        @pl.loop(0, chunks)
        def _(chunk):
            @pl.when(at < wave)
            def _():
                send(n - wave + at, chunk, 0, at > 0)

            @pl.when(far < wave)
            def _():
                send(wave - 1 - far, chunk, 1, far > 0)

    @pl.loop(0, chunks)
    def _(chunk):
        def put(cols, value):
            result[chunk, :, cols] = value

        product(at, chunk, put)

    for chunk in range(chunks):

        @pl.when(at > 0)
        def _():
            scatter.arrive(chunk, at)
            result[chunk] += held[chunk, at].astype(jnp.float32)

        @pl.when(far > 0)
        def _():
            scatter.arrive(chunk, n)
            result[chunk] += held[chunk, n].astype(jnp.float32)

        scatter.drain(chunk)


def multiply_scatter(n, left, right, first, collective_id, name):
    _, chunks, rows, depth = left.shape
    width = right.shape[0]
    vmem = pl.BlockSpec(memory_space=pltpu.VMEM)
    hbm = pl.BlockSpec(memory_space=pl.ANY)
    return pl.pallas_call(
        functools.partial(multiply_scatter_kernel, n, first),
        name=name,
        out_shape=jax.ShapeDtypeStruct((chunks, rows, width), jnp.float32),
        in_specs=[vmem, hbm],
        out_specs=vmem,
        scratch_shapes=[
            pltpu.VMEM((chunks, n, rows, width), jnp.bfloat16),
            pltpu.VMEM((chunks, n + 1, rows, width), jnp.bfloat16),
            pltpu.VMEM(right.shape, right.dtype),
            pltpu.SemaphoreType.DMA((chunks, 2, n)),
            pltpu.SemaphoreType.DMA((chunks, n + 1)),
            pltpu.SemaphoreType.DMA((1,)),
        ],
        compiler_params=pltpu.CompilerParams(
            collective_id=collective_id, has_side_effects=True, vmem_limit_bytes=56 << 20
        ),
    )(left, right)


def on_device(
    sizes,
    block_in,
    cotangent,
    attention_matrix,
    attention_first_moment,
    attention_second_moment,
    mlp_weight,
    first_mlp,
    second_mlp,
    norm_weight,
    first_norm,
    second_norm,
):
    n_fsdp, n_seq, n_mlp = sizes
    count = n_fsdp * n_seq * n_mlp
    sequence_count, token_length, feat_width = block_in.shape
    row_count = sequence_count * token_length
    seq_rows = n_seq * row_count
    query_total_width = QUERY_HEADS * HEAD_SIZE
    key_value_width = KEY_VALUE_HEADS * HEAD_SIZE
    group = QUERY_HEADS // KEY_VALUE_HEADS
    heads = QUERY_HEADS // n_seq
    kv_heads = KEY_VALUE_HEADS // n_seq
    own_q = heads * HEAD_SIZE
    own_kv = kv_heads * HEAD_SIZE
    own_width = own_q + 2 * own_kv
    share = attention_matrix.shape[0]

    tok_rows = block_in.reshape(row_count, feat_width)
    upstream = cotangent.reshape(row_count, feat_width)

    gain_tile = jnp.zeros((1, 8, 128), jnp.float32)
    gain_tile = gain_tile.at[0, : norm_weight.shape[0], : norm_weight.shape[1]].set(
        norm_weight.astype(jnp.bfloat16).astype(jnp.float32)
    )
    attn_bf = attention_matrix.astype(jnp.bfloat16)
    own_o = query_total_width // n_seq
    cuts = (query_total_width, key_value_width, key_value_width, query_total_width)
    pieces, start = [], 0
    for cut in cuts:
        pieces.append(attn_bf[:, start : start + cut].reshape(share, n_seq, cut // n_seq))
        start += cut
    head_parts = jnp.transpose(jnp.concatenate(pieces, axis=2), (1, 0, 2))
    gain_tiles, head_cols = exchange(sizes, gain_tile, head_parts, 0)
    gains = gain_tiles[:, : norm_weight.shape[0], : norm_weight.shape[1]]
    factor = 1.0 + jnp.transpose(gains, (1, 0, 2)).reshape(norm_weight.shape[0], feat_width)
    all_width = own_width + own_o
    w_heads = lax.all_gather(head_cols, ("fsdp", "mlp"), axis=0, tiled=False)
    w_heads = jnp.transpose(
        w_heads.reshape(n_fsdp, n_mlp, n_seq, share, all_width), (0, 2, 1, 3, 4)
    ).reshape(feat_width, all_width)

    inverse_in = scale_rows(tok_rows)
    normed_in = (tok_rows * inverse_in * factor[0]).astype(jnp.bfloat16)
    part_shape = (row_chunks, row_count // row_chunks, feat_width)
    whole_xn = gather_rows(n_seq, normed_in.reshape(part_shape), 4).reshape(seq_rows, feat_width)
    qkv = jnp.dot(
        whole_xn, w_heads[:, :own_width], preferred_element_type=jnp.float32
    ).astype(jnp.bfloat16)
    query_h = qkv[:, :own_q].reshape(sequence_count, seq_rows, heads, HEAD_SIZE)
    key_h = jnp.repeat(
        qkv[:, own_q : own_q + own_kv].reshape(sequence_count, seq_rows, kv_heads, HEAD_SIZE),
        group,
        axis=2,
    )
    value_h = jnp.repeat(
        qkv[:, own_q + own_kv :].reshape(sequence_count, seq_rows, kv_heads, HEAD_SIZE),
        group,
        axis=2,
    )
    block_rows = min(512, seq_rows)
    mixed_h, totals, saved_state = attend(query_h, key_h, value_h, block_rows)
    mixed_own = mixed_h.reshape(seq_rows, own_q)
    projected = multiply_scatter(
        n_seq,
        mixed_own.reshape((n_seq,) + part_shape[:2] + (own_q,)),
        w_heads,
        own_width,
        5,
        "project",
    ).reshape(row_count, feat_width)
    inverse_one = scale_rows(projected)
    middle = tok_rows + projected * inverse_one * factor[1]
    inverse_two = scale_rows(middle)
    normed_mid = (middle * inverse_two * factor[2]).astype(jnp.bfloat16)
    whole_mlp = lax.all_gather(mlp_weight.astype(jnp.bfloat16), "fsdp", axis=1, tiled=True)
    mlp_parts = (whole_mlp[0], whole_mlp[1], whole_mlp[2])
    chunk_shape = (mlp_chunks, row_count // mlp_chunks, feat_width)
    hidden = whole_mlp.shape[2]
    mlp_rows, hidden_activation, gelu_rows, slope_rows, ffn_out = mlp_half(
        True, n_seq, normed_mid.reshape(chunk_shape), mlp_parts, (), 2
    )
    ffn_out = ffn_out.reshape(row_count, feat_width)
    inverse_three = scale_rows(ffn_out)
    block_out = middle + ffn_out * inverse_three * factor[3]
    dffn, gain_three = norm_back(ffn_out, inverse_three, factor[3], upstream)
    dffn_rows, gate_gradient, up_gradient_half, dnormed_mid = mlp_half(
        False,
        n_seq,
        dffn.astype(jnp.bfloat16).reshape(chunk_shape),
        mlp_parts,
        (gelu_rows, slope_rows),
        3,
    )
    dnormed_mid = dnormed_mid.reshape(row_count, feat_width)
    mlp_rows = mlp_rows.reshape(-1, feat_width)
    dffn_rows = dffn_rows.reshape(-1, feat_width)
    hidden_activation = hidden_activation.reshape(-1, hidden)
    gate_gradient = gate_gradient.reshape(-1, hidden)
    up_gradient_half = up_gradient_half.reshape(-1, hidden)
    grad_gate = jnp.einsum("rd,rf->df", mlp_rows, gate_gradient, preferred_element_type=jnp.float32)
    grad_up = jnp.einsum(
        "rd,rf->df", mlp_rows, up_gradient_half, preferred_element_type=jnp.float32
    )
    grad_down = jnp.einsum(
        "rd,rf->df", dffn_rows, hidden_activation, preferred_element_type=jnp.float32
    )
    mlp_grad = lax.psum_scatter(
        jnp.stack([grad_gate, grad_up, grad_down]).astype(jnp.bfloat16),
        "fsdp",
        scatter_dimension=1,
        tiled=True,
    ).astype(jnp.float32)
    dmid_part, gain_two = norm_back(middle, inverse_two, factor[2], dnormed_mid)
    dmiddle = upstream + dmid_part
    dproj, gain_one = norm_back(projected, inverse_one, factor[1], dmiddle)
    dproj_bf = dproj.astype(jnp.bfloat16)
    whole_dproj = gather_rows(n_seq, dproj_bf.reshape(part_shape), 6).reshape(seq_rows, feat_width)
    dmixed_h = (
        jnp.dot(whole_dproj, w_heads[:, own_width:], preferred_element_type=jnp.float32)
        .astype(jnp.bfloat16)
        .reshape(sequence_count, seq_rows, heads, HEAD_SIZE)
    )
    dquery_h, dkey_h, dvalue_h = attend_back(
        query_h, key_h, value_h, mixed_h, totals, dmixed_h, block_rows
    )

    def group_sum(values):
        return (
            jnp.sum(
                values.astype(jnp.float32).reshape(seq_rows, kv_heads, group, HEAD_SIZE), axis=2
            )
            .astype(jnp.bfloat16)
            .reshape(seq_rows, own_kv)
        )

    dqkv = jnp.concatenate(
        [dquery_h.reshape(seq_rows, own_q), group_sum(dkey_h), group_sum(dvalue_h)], axis=1
    )
    dnormed_in = multiply_scatter(
        n_seq,
        dqkv.reshape((n_seq,) + part_shape[:2] + (own_width,)),
        w_heads,
        0,
        7,
        "input_gradient",
    ).reshape(row_count, feat_width)
    grad_heads = jnp.concatenate(
        [
            jnp.einsum("tr,tc->rc", whole_xn, dqkv, preferred_element_type=jnp.float32).astype(
                jnp.bfloat16
            ),
            jnp.einsum(
                "tr,tc->rc", whole_dproj, mixed_own, preferred_element_type=jnp.float32
            ).astype(jnp.bfloat16),
        ],
        axis=1,
    )
    grad_heads = jnp.transpose(
        grad_heads.reshape(n_fsdp, n_seq, n_mlp, share, all_width), (0, 2, 1, 3, 4)
    ).reshape(feat_width, all_width)
    grad_heads = lax.psum_scatter(grad_heads, ("fsdp", "mlp"), scatter_dimension=0, tiled=True)
    dinput_part, gain_zero = norm_back(tok_rows, inverse_in, factor[0], dnormed_in)
    input_grad = dmiddle + dinput_part

    gain_sums = jnp.stack([gain_zero, gain_one, gain_two, gain_three])
    gain_parts = jnp.transpose(gain_sums.reshape(4, count, feat_width // count), (1, 0, 2))
    gain_parts = jnp.pad(gain_parts, ((0, 0), (0, 4), (0, 128 - feat_width // count)))
    gain_tiles, grad_cols = exchange(
        sizes, gain_parts, grad_heads.reshape(n_seq, share, all_width), 1
    )
    norm_grad = jnp.sum(gain_tiles, axis=0)[: norm_weight.shape[0], : norm_weight.shape[1]]
    pieces, start = [], 0
    for cut in cuts:
        piece = grad_cols[:, :, start : start + cut // n_seq]
        pieces.append(jnp.transpose(piece, (1, 0, 2)).reshape(share, cut))
        start += cut // n_seq
    attn_grad = jnp.concatenate(pieces, axis=1).astype(jnp.float32)

    attn_new, first_attn_new, second_attn_new = adam_update(
        attention_matrix, attn_grad, attention_first_moment, attention_second_moment, decay_rate
    )
    mlp_new, first_mlp_new, second_mlp_new = adam_update(
        mlp_weight, mlp_grad, first_mlp, second_mlp, decay_rate
    )
    norm_new, first_norm_new, second_norm_new = adam_update(
        norm_weight, norm_grad, first_norm, second_norm, 0.0
    )
    return (
        block_out.reshape(block_in.shape),
        input_grad.reshape(block_in.shape),
        attn_grad,
        attn_new,
        first_attn_new,
        second_attn_new,
        mlp_grad,
        mlp_new,
        first_mlp_new,
        second_mlp_new,
        norm_grad,
        norm_new,
        first_norm_new,
        second_norm_new,
    )


def solution(mesh):
    sizes = (mesh.shape["fsdp"], mesh.shape["seq"], mesh.shape["mlp"])
    fits = KEY_VALUE_HEADS % sizes[1] == 0 and sizes[2] == 2
    body = functools.partial(on_device, sizes) if fits else on_device_generic
    placed = (
        P(("fsdp", "mlp"), "seq", None),
        P(("fsdp", "mlp"), "seq", None),
        P(("fsdp", "seq", "mlp"), None),
        P(("fsdp", "seq", "mlp"), None),
        P(("fsdp", "seq", "mlp"), None),
        P(None, "fsdp", ("seq", "mlp")),
        P(None, "fsdp", ("seq", "mlp")),
        P(None, "fsdp", ("seq", "mlp")),
        P(None, ("fsdp", "seq", "mlp")),
        P(None, ("fsdp", "seq", "mlp")),
        P(None, ("fsdp", "seq", "mlp")),
    )
    return jax.shard_map(
        body,
        mesh=mesh,
        in_specs=placed,
        out_specs=(
            P(("fsdp", "mlp"), "seq", None),
            P(("fsdp", "mlp"), "seq", None),
            P(("fsdp", "seq", "mlp"), None),
            P(("fsdp", "seq", "mlp"), None),
            P(("fsdp", "seq", "mlp"), None),
            P(("fsdp", "seq", "mlp"), None),
            P(None, "fsdp", ("seq", "mlp")),
            P(None, "fsdp", ("seq", "mlp")),
            P(None, "fsdp", ("seq", "mlp")),
            P(None, "fsdp", ("seq", "mlp")),
            P(None, ("fsdp", "seq", "mlp")),
            P(None, ("fsdp", "seq", "mlp")),
            P(None, ("fsdp", "seq", "mlp")),
            P(None, ("fsdp", "seq", "mlp")),
        ),
        check_vma=False,
    )
```
